32 devices in a mesh: cuts: 16 (over z, y, x), circ: 2 (over core).
Axes of the slice: x: 2, y: 2, z: 4, core: 2. Of those that a mesh axis runs over, the one named last changes fastest.
Arguments:
- sources: bfloat16 [16, 8, 2, 16, 1024], P('cuts', None, 'circ'), may hold values from -6 to 6
- block_inverse: bfloat16 [2, 1024, 1024], P('circ'), may hold values from -0.0115625 to 0.92
- memory_factor: float32 [16, 2, 1024], P('cuts', 'circ'), may hold values from 0.5 to 1
- coupling_target: int32 [2, 4], P('circ'), may hold values from 0 to 1, as said below
- coupling_weight: bfloat16 [2, 4, 128, 1024], P('circ'), may hold values from -0.09375 to 0.09375
- coarse_decay: float32 [16, 2, 1024], P('cuts', 'circ'), may hold values from 0.2 to 0.995
- initial_state: float32 [2, 16, 1024], P('circ'), may hold values from -6 to 6
Outputs:
- slice_starts: float32 [16, 2, 16, 1024], P('cuts', 'circ')
- waveform: bfloat16 [16, 8, 2, 16, 1024], P('cuts', None, 'circ')
The draws below stay inside these ranges and needn't reach their ends.
Inputs may be any that keep to these rules, and one draw needn't show every extreme that they name: `coupling_target`: row j names 4 subcircuits, j itself among them possibly; a row may name one subcircuit twice.
All inputs are finite; a program needn't handle non-finite values.
Results may differ from the reference program's by a relative error of at most 0.007.
Values sent between devices are 32-bit elements; how exact they have to be, the bound alone decides.
A program may use at most 64 MiB of HBM per device.

```python
import math
import jax
import jax.numpy as jnp
from jax import lax

CIRCUIT_NODES = 1024
PORTS = 128
SCEN = 16
STEPS = 8
SWEEPS = 3
ITERS = 2
KC = 4
SUB_DEV = 1
SUBCIRCUIT_COUNT = 2
TIME_SLICES = 16
N_CIRC = 2


def draw_block_inverse(key, part):
    key_diag = jax.random.fold_in(key, 11)
    key_off = jax.random.fold_in(key, 12)
    spread = 0.12 * CIRCUIT_NODES ** (-0.5)
    diagonal = jnp.exp(jax.random.uniform(key_diag, (SUBCIRCUIT_COUNT, CIRCUIT_NODES), jnp.float32, jnp.log(0.3), jnp.log(0.85)))
    offdiag = jnp.clip(jax.random.normal(key_off, (SUBCIRCUIT_COUNT, CIRCUIT_NODES, CIRCUIT_NODES), jnp.float32), -3.0, 3.0) * spread
    identity = jnp.eye(CIRCUIT_NODES, dtype=jnp.float32)
    return (offdiag + diagonal[:, :, None] * identity[None]).astype(jnp.bfloat16)


def draw_coupling_target(key, part):
    targets = jax.random.randint(jax.random.fold_in(key, 21), (SUBCIRCUIT_COUNT, KC), 0, SUBCIRCUIT_COUNT)
    return targets.astype(jnp.int32)


def draw_coarse_decay(key, part):
    random_key_list = [jax.random.fold_in(key, 31 + offset) for offset in range(5)]
    slow_share = 0.5
    slow_mask = jax.random.uniform(random_key_list[0], (SUBCIRCUIT_COUNT, CIRCUIT_NODES), jnp.float32) < slow_share
    sluggish_rate = jax.random.uniform(random_key_list[1], (TIME_SLICES, SUBCIRCUIT_COUNT, CIRCUIT_NODES), jnp.float32, 0.97, 0.995)
    fast_rate = jax.random.uniform(random_key_list[2], (TIME_SLICES, SUBCIRCUIT_COUNT, CIRCUIT_NODES), jnp.float32, 0.2, 0.6)
    spike_slices = jax.random.randint(random_key_list[3], (3,), 0, TIME_SLICES)
    spike_active = jnp.any(jnp.arange(TIME_SLICES)[:, None] == spike_slices[None, :], axis=1)
    spike_multiplier = jax.random.uniform(random_key_list[4], (TIME_SLICES, SUBCIRCUIT_COUNT, CIRCUIT_NODES), jnp.float32, 0.5, 0.8)
    sluggish_rate = jnp.where(spike_active[:, None, None], sluggish_rate * spike_multiplier, sluggish_rate)
    return jnp.where(slow_mask[None], sluggish_rate, fast_rate).astype(jnp.float32)


def level_of(key, dims, cuts, low, largest):
    def one(position, blocks):
        steps = jax.random.uniform(jax.random.fold_in(jax.random.fold_in(key, 6), position), (blocks,), jnp.float32, low / len(cuts), largest / len(cuts))
        return jnp.repeat(jnp.exp(steps), dims[position] // blocks).reshape((-1,) + (1,) * (len(dims) - position - 1))

    loudness = one(*cuts[0])
    for cut in cuts[1:]:
        loudness = loudness * one(*cut)
    return loudness


def normal_values(own_key, extent, deviation, most, pieces=(), held_as=jnp.bfloat16):
    array = jax.random.normal(own_key, extent, jnp.float32) * deviation
    if len(pieces) > 0:
        array = level_of(own_key, extent, pieces, -0.22, 0.18) * array
    return jnp.clip(array, min=-most, max=most).astype(held_as)


def setup_inputs(seed: int = 0) -> dict:
    streams_of = jax.random.split(jax.random.key(seed), 8)
    sources = normal_values(streams_of[0], (TIME_SLICES, STEPS, SUBCIRCUIT_COUNT, SCEN, CIRCUIT_NODES), 1.0, 6.0, ((0, 16), (2, 2)))
    block_inverse = draw_block_inverse(jax.random.fold_in(streams_of[7], 71), 0)
    memory_factor = jnp.clip(jnp.exp(math.log(1.0) - 0.6931472 * jax.random.uniform(streams_of[2], (TIME_SLICES, SUBCIRCUIT_COUNT, CIRCUIT_NODES), jnp.float32) ** level_of(streams_of[2], (TIME_SLICES, SUBCIRCUIT_COUNT, CIRCUIT_NODES), ((0, 16), (1, 2)), -0.2, 0.2)), 0.5, 1.0)
    coupling_target = draw_coupling_target(jax.random.fold_in(streams_of[7], 71), 0)
    coupling_weight = normal_values(streams_of[4], (SUBCIRCUIT_COUNT, KC, PORTS, CIRCUIT_NODES), (4 * CIRCUIT_NODES) ** -0.5, 0.09375, ((0, 2),))
    coarse_decay = draw_coarse_decay(jax.random.fold_in(streams_of[7], 71), 0)
    initial_state = normal_values(streams_of[6], (SUBCIRCUIT_COUNT, SCEN, CIRCUIT_NODES), 1.0, 6.0, ((0, 2),), jnp.float32)
    return {"sources": sources, "block_inverse": block_inverse, "memory_factor": memory_factor, "coupling_target": coupling_target, "coupling_weight": coupling_weight, "coarse_decay": coarse_decay, "initial_state": initial_state}


highest = lax.Precision.HIGHEST


def to_low(values):
    return lax.optimization_barrier(values.astype(jnp.bfloat16)).astype(jnp.float32)


def run_chain(decay_rate, coarse_terms, initial):
    def advance(carried, paired):
        rate_now, extra_term = paired
        return rate_now[:, None, :] * carried + extra_term, carried

    unused, starts = lax.scan(advance, initial, (decay_rate, coarse_terms))
    return starts


def coupling_inflow(wave_now, coupling_target, weights_wide):
    wave_low = to_low(wave_now)
    contrib = jnp.einsum('skpn,tsqn->sktqp', weights_wide, wave_low, precision=highest)
    owners = (coupling_target[:, :, None] == jnp.arange(SUBCIRCUIT_COUNT, dtype=jnp.int32)[None, None, :]).astype(jnp.float32)
    grouped = contrib.reshape((N_CIRC, SUB_DEV) + contrib.shape[1:])
    owner_groups = owners.reshape((N_CIRC, SUB_DEV) + owners.shape[1:])
    partial_sums = jnp.einsum('dskg,dsktqp->dgtqp', owner_groups, grouped, precision=highest)
    return jnp.sum(partial_sums, axis=0)


def fine_slice(begin_state, slice_sources, factor, block_wide, coupling_target, weights_wide):
    wave_now = jnp.broadcast_to(begin_state, (STEPS,) + begin_state.shape)
    for sweep_index in range(SWEEPS):
        inflow = coupling_inflow(wave_now, coupling_target, weights_wide)
        previous = begin_state
        columns = []
        for step_index in range(STEPS):
            drive_term = factor[:, None, :] * previous + slice_sources[step_index].astype(jnp.float32)
            drive_term = drive_term.at[:, :, :PORTS].add(inflow[:, step_index])
            previous = jnp.einsum('smn,sqn->sqm', block_wide, to_low(drive_term), precision=highest)
            columns.append(previous)
        wave_now = jnp.stack(columns)
    return wave_now


def reference(sources, block_inverse, memory_factor, coupling_target, coupling_weight, coarse_decay, initial_state):
    block_wide = block_inverse.astype(jnp.float32)
    weights_wide = coupling_weight.astype(jnp.float32)
    coarse_load = jnp.mean(sources.astype(jnp.float32), axis=1)
    begin_all = run_chain(coarse_decay, coarse_load, initial_state)
    waves = None
    for iteration in range(ITERS):
        def one_slice(packed):
            begin_state, slice_sources, factor = packed
            return fine_slice(begin_state, slice_sources, factor, block_wide, coupling_target, weights_wide)

        waves = lax.map(one_slice, (begin_all, sources, memory_factor))
        correction = waves[:, -1] - coarse_decay[:, :, None, :] * begin_all
        begin_all = run_chain(coarse_decay, correction, initial_state)
    return begin_all, waves.astype(jnp.bfloat16)
```

```python
import functools

import jax
import jax.numpy as jnp
from jax import lax
from jax.experimental import pallas as pl
from jax.experimental.pallas import tpu as pltpu
from jax.sharding import PartitionSpec as P

SWEEPS = 3
ITERS = 2
MESH = pl.DeviceIdType.MESH
F32 = jnp.float32
BF16 = jnp.bfloat16
LANE = 128


def dot(a, b):
    return jnp.dot(a.astype(BF16), b.astype(BF16), preferred_element_type=F32)


def kernel(
    cuts,
    circ,
    steps,
    fused,
    src_in,
    inv_in,
    mem_in,
    tgt_in,
    cw_in,
    dec_in,
    init_in,
    start_ref,
    wave_out,
    src_ref,
    inv_ref,
    mem_ref,
    tgt_ref,
    cw_ref,
    dec_ref,
    init_ref,
    wave_ref,
    sem_in,
    sem_inv,
    sem_out,
    inv_t,
    pow1,
    pow2,
    pow4,
    port_t,
    resp,
    k_all,
    k_sum,
    k_me,
    own,
    free,
    terms_buf,
    gather_buf,
    chain_buf,
    state_buf,
    decay_buf,
    u_buf,
    y_buf,
    part_buf,
    inflow_buf,
    send1,
    recv1,
    send2,
    recv2,
    send_d,
    recv_d,
    send_k,
    recv_k,
    send_u,
    recv_u,
    send_y,
    recv_y,
    send_x,
    recv_x,
):
    scope = jax.named_scope
    n = lax.axis_index("cuts")
    me = lax.axis_index("circ")
    nodes = inv_ref.shape[0]
    scen = init_ref.shape[0]
    rows = src_ref.shape[0]
    blocks, ports = cw_ref.shape[0], cw_ref.shape[1]
    cols = nodes // LANE
    base = (cuts - cols) // 2
    piece = n - base
    owner = jnp.logical_and(n >= base, n < base + cols)
    lane = pl.multiple_of(piece * LANE, LANE)
    mine = pl.ds(pl.multiple_of(me * ports, ports), ports)
    last = rows - scen

    def cut(k):
        return lax.rem(n + k, cuts)

    def peer(k):
        return lax.rem(me + k, circ)

    barrier = pltpu.get_barrier_semaphore()

    @pl.loop(1, cuts)
    def _(k):
        pl.semaphore_signal(barrier, inc=1, device_id=(cut(k), me), device_id_type=MESH)

    for k in range(1, circ):
        pl.semaphore_signal(barrier, inc=1, device_id=(n, peer(k)), device_id_type=MESH)

    def load(k, a, b):
        return pltpu.make_async_copy(a, b, sem_in.at[k])

    first_loads = [load(0, src_in, src_ref), load(1, mem_in, mem_ref)]
    last_loads = [
        load(2, dec_in, dec_ref),
        load(3, tgt_in, tgt_ref),
        load(4, cw_in, cw_ref),
        load(5, init_in, init_ref),
    ]
    strips = []
    for c in range(cols):
        at = pl.ds(c * LANE, LANE)
        strips.append(pltpu.make_async_copy(inv_in.at[at], inv_ref.at[at], sem_inv.at[c]))
    for copy in first_loads + strips + last_loads:
        copy.start()

    def term_copy(c, k, dest, source):
        return pltpu.make_async_remote_copy(
            src_ref=terms_buf.at[c, k],
            dst_ref=gather_buf.at[c, source],
            send_sem=send1.at[c, k],
            recv_sem=recv1.at[c, source],
            device_id=(dest, me),
            device_id_type=MESH,
        )

    def decay_copy(k, dest, source):
        return pltpu.make_async_remote_copy(
            src_ref=dec_ref.at[:, pl.ds(k * LANE, LANE)],
            dst_ref=decay_buf.at[source],
            send_sem=send_d.at[k],
            recv_sem=recv_d.at[source],
            device_id=(dest, me),
            device_id_type=MESH,
        )

    def state_copy(c, dest, other, k):
        return pltpu.make_async_remote_copy(
            src_ref=chain_buf.at[c, dest],
            dst_ref=state_buf.at[c, k],
            send_sem=send2.at[c, dest],
            recv_sem=recv2.at[c, k],
            device_id=(other, me),
            device_id_type=MESH,
        )

    def sends_to(dest):
        return jnp.logical_and(n != dest, n < cuts - 1)

    def chain_send(c, terms):
        for k in range(cols):
            terms_buf[c, k] = terms[:, k * LANE : (k + 1) * LANE]
        for k in range(cols):

            @pl.when(sends_to(base + k))
            def _():
                term_copy(c, k, base + k, n).start()
                if c == 0:
                    decay_copy(k, base + k, n).start()

    def chain_turn(c):
        @pl.when(owner)
        def _():
            if c == 0:
                decay_buf[n] = dec_ref[:, pl.ds(lane, LANE)]
            gather_buf[c, n] = terms_buf[c, piece]
            state = init_ref[:, pl.ds(lane, LANE)]
            for s in range(cuts):
                chain_buf[c, s] = state

                @pl.when(n != s)
                def _():
                    state_copy(c, s, s, piece).start()
                    if s < cuts - 1:
                        term_copy(c, 0, s, s).wait_recv()
                        if c == 0:
                            decay_copy(0, s, s).wait_recv()

                if s < cuts - 1:
                    state = decay_buf[s] * state + gather_buf[c, s]
            state_buf[c, piece] = chain_buf[c, n]

    def chain_end(c):
        for k in range(cols):

            @pl.when(n != base + k)
            def _():
                state_copy(c, 0, base + k, k).wait_recv()

        return jnp.concatenate([state_buf[c, k] for k in range(cols)], axis=1)

    def drain(c):
        for k in range(cols):

            @pl.when(sends_to(base + k))
            def _():
                term_copy(c, k, base + k, n).wait_send()
                if c == 0:
                    decay_copy(k, base + k, n).wait_send()

        @pl.when(owner)
        def _():
            @pl.loop(1, cuts)
            def _(k):
                d = cut(k)
                state_copy(c, d, d, piece).wait_send()

    def swap_copy(ref, send, recv, k, source):
        return pltpu.make_async_remote_copy(
            src_ref=ref.at[me],
            dst_ref=ref.at[source],
            send_sem=send.at[k - 1],
            recv_sem=recv.at[source],
            device_id=(n, peer(k)),
            device_id_type=MESH,
        )

    class Swap:
        def __init__(self, *refs):
            self.refs = refs

        def start(self):
            for k in range(1, circ):
                swap_copy(*self.refs, k, me).start()

        def wait(self):
            for k in range(1, circ):
                swap_copy(*self.refs, k, peer(k)).wait_recv()

        def drain(self):
            for k in range(1, circ):
                swap_copy(*self.refs, k, me).wait_send()

    def current_copy(e, height, k, source):
        return pltpu.make_async_remote_copy(
            src_ref=part_buf.at[e, peer(k), pl.ds(0, height)],
            dst_ref=inflow_buf.at[e, source, pl.ds(0, height)],
            send_sem=send_x.at[e, k - 1],
            recv_sem=recv_x.at[e, source],
            device_id=(n, peer(k)),
            device_id_type=MESH,
        )

    def exchange_start(e, partial):
        height = partial.shape[0]
        for g in range(circ):
            part_buf[e, g, 0:height] = partial[:, g * ports : (g + 1) * ports]
        for k in range(1, circ):
            current_copy(e, height, k, me).start()

    def exchange_end(e, height):
        total = part_buf[e, me, 0:height]
        for k in range(1, circ):
            current_copy(e, height, k, peer(k)).wait_recv()
            total = total + inflow_buf[e, peer(k), 0:height]
        return total

    def exchange_drain(e, height):
        for k in range(1, circ):
            current_copy(e, height, k, me).wait_send()

    wide = min(256, nodes)

    def product(out, left, right):
        for at in range(0, nodes, wide):
            out[:, at : at + wide] = dot(left[...], right[:, at : at + wide]).astype(BF16)

    with scope("w_src"):
        for copy in first_loads:
            copy.wait()
    with scope("mean"):
        mean = src_ref[0:scen].astype(F32)
        for t in range(1, steps):
            mean = mean + src_ref[t * scen : (t + 1) * scen].astype(F32)
        mean = mean * (1.0 / steps)
        factor = jnp.broadcast_to(mem_ref[...], (LANE, nodes)).T
    for c in range(cols):
        at = slice(c * LANE, (c + 1) * LANE)
        with scope("w_inv"):
            strips[c].wait()
        turned = inv_ref[at, :].T
        inv_t[:, at] = turned
        pow1[:, at] = (turned.astype(F32) * factor).astype(BF16)
    with scope("w_rest"):
        for copy in last_loads:
            copy.wait()
    with scope("w_barrier"):
        pl.semaphore_wait(barrier, cuts - 1 + circ - 1)
    chain_send(0, mean)

    with scope("port_t"):
        for g in range(circ):
            summed = jnp.zeros((ports, nodes), F32)
            for b in range(blocks):
                share = jnp.where(tgt_ref[0, b] == g, 1.0, 0.0).astype(F32)
                summed = summed + share * cw_ref[b].astype(F32)
            port_t[:, g * ports : (g + 1) * ports] = summed.astype(BF16).T

    def one_step(values):
        exact = mem_ref[...] * values
        high = exact.astype(BF16)
        low = (exact - high.astype(F32)).astype(BF16)
        both = dot(jnp.concatenate([high, low], axis=0), inv_t[...])
        return both[: values.shape[0]] + both[values.shape[0] :]

    with scope("pow2"):
        product(pow2, pow1, pow1)
    with scope("own0"):
        own[...] = dot(src_ref[...], inv_t[...])
        resp[0:ports] = inv_t[0:ports]

    with scope("turn0"):
        chain_turn(0)

    with scope("own1"):
        own[scen:] = own[scen:] + one_step(own[: rows - scen])
        resp[ports : 2 * ports] = dot(resp[0:ports], pow1[...]).astype(BF16)

    def beside(left, low, power):
        count = left.shape[0]
        both = dot(jnp.concatenate([left, resp[low * ports : (low + 2) * ports]], axis=0), power)
        resp[(low + 2) * ports : (low + 4) * ports] = both[count:].astype(BF16)
        return both[:count]

    with scope("own2"):
        own[2 * scen :] = own[2 * scen :] + beside(own[: rows - 2 * scen].astype(BF16), 0, pow2[...])
    with scope("own4"):
        ahead = beside(own[: rows - 4 * scen].astype(BF16), 2, pow2[...])
        own[4 * scen :] = own[4 * scen :] + beside(ahead.astype(BF16), 4, pow2[...])

    if fused:
        k_swap = Swap(k_all, send_k, recv_k)
        u_swaps = [Swap(u_buf.at[i], send_u.at[i], recv_u.at[i]) for i in range(ITERS)]
        y_swaps = [Swap(y_buf.at[i], send_y.at[i], recv_y.at[i]) for i in range(ITERS)]

        def take(j):
            width = circ * ports
            total = jnp.zeros((ports, width), F32)
            for t in range(steps):
                total = total + k_all[j, t * ports : (t + 1) * ports]
                k_sum[pl.ds(pl.multiple_of(j * ports, ports), ports), t * width : (t + 1) * width] = (
                    total.astype(BF16)
                )
            span = steps * ports
            k_me[pl.ds(pl.multiple_of(j * span, span), span), :] = k_all[j, :, mine].astype(BF16)

    with scope("port_resp"):
        heard = dot(resp[...], port_t[...])
        if fused:
            k_all[me] = heard
            k_swap.start()
            take(me)
        else:
            k_me[...] = heard.astype(BF16)

    def shifted(low):
        columns = [low]
        for lag in range(1, steps):
            columns.append(
                jnp.concatenate(
                    [jnp.zeros((lag * scen, ports), BF16), low[: rows - lag * scen]], axis=0
                )
            )
        return columns

    def by_lag(currents):
        return jnp.concatenate(shifted(currents.astype(BF16)), axis=1)

    def end_lags(currents):
        low = currents.astype(BF16)
        return jnp.concatenate(
            [low[(steps - 1 - lag) * scen : (steps - lag) * scen] for lag in range(steps)], axis=1
        )

    with scope("end0"):
        begin = chain_end(0)
    for iteration in range(ITERS):
        first = iteration * SWEEPS
        with scope("free"):
            outflow = dot(begin, port_t[...])
            if fused:
                u_buf[iteration, me] = outflow
                u_swaps[iteration].start()
            else:
                exchange_start(first, outflow)
            v0 = begin.astype(BF16)
            v1 = one_step(begin)
            v2 = dot(v0, pow2[...])
            v12 = jnp.concatenate([v1, v2], axis=0).astype(BF16)
            v34 = dot(v12, pow2[...])
            if iteration == 0:
                v56 = dot(v34, pow2[...])
                v78 = dot(v56, pow2[...])
                v58 = jnp.concatenate([v56, v78], axis=0)
            else:
                v14 = jnp.concatenate([v12, v34.astype(BF16)], axis=0)
                v58 = dot(v14, pow4[...])
            free[0:scen] = own[0:scen] + v1
            free[scen : 2 * scen] = own[scen : 2 * scen] + v2
            free[2 * scen : 4 * scen] = own[2 * scen : 4 * scen] + v34
            free[4 * scen :] = own[4 * scen :] + v58
            seen = dot(free[...], port_t[...])
        if fused:
            with scope("y_start"):
                y_buf[iteration, me] = seen
                y_swaps[iteration].start()
            with scope("w_k"):
                if iteration == 0:
                    k_swap.wait()
                    for k in range(1, circ):
                        take(peer(k))
            with scope("w_u"):
                u_swaps[iteration].wait()
            with scope("ku"):
                inflow = outflow
                for k in range(1, circ):
                    inflow = inflow + u_buf[iteration, peer(k)]
                raised = dot(inflow, k_sum[...])
                width = circ * ports
                raised = jnp.concatenate(
                    [raised[:, t * width : (t + 1) * width] for t in range(steps)], axis=0
                )
            with scope("w_y"):
                y_swaps[iteration].wait()
            with scope("sweep"):
                total = seen
                direct = y_buf[iteration, me, :, mine]
                for k in range(1, circ):
                    total = total + y_buf[iteration, peer(k)]
                    direct = direct + y_buf[iteration, peer(k), :, mine]
                second = (total + raised).astype(BF16)
                columns = []
                for g in range(circ):
                    columns += shifted(second[:, g * ports : (g + 1) * ports])
                current = direct + dot(jnp.concatenate(columns, axis=1), k_me[...])
        else:
            current = exchange_end(first, scen)
            current = jnp.concatenate([current] * steps, axis=0)
            for sweep in range(1, SWEEPS):
                exchange_start(first + sweep, seen + dot(by_lag(current), k_me[...]))
                current = exchange_end(first + sweep, rows)
        with scope("final"):
            final = free[last:] + dot(end_lags(current), resp[...])
        with scope("send"):
            chain_send(iteration + 1, final - dec_ref[...] * begin)
        if iteration < ITERS - 1:
            with scope("pow4"):
                product(pow4, pow2, pow2)
        else:
            with scope("wave"):
                wave = free[...] + dot(by_lag(current), resp[...])
                wave_ref[...] = wave.astype(BF16)
                result = pltpu.make_async_copy(wave_ref, wave_out, sem_out)
                result.start()
        with scope("turn"):
            chain_turn(iteration + 1)
        with scope("end"):
            begin = chain_end(iteration + 1)
    with scope("out"):
        start_ref[...] = begin
        result.wait()

    with scope("drain"):
        for c in range(ITERS + 1):
            drain(c)
        if fused:
            k_swap.drain()
            for swap in u_swaps + y_swaps:
                swap.drain()
        else:
            for e in range(SWEEPS * ITERS):
                exchange_drain(e, scen if e % SWEEPS == 0 else rows)


def hand_over(start_in, wave_in, start_out, wave_out):
    start_out[...] = start_in[...]
    wave_out[...] = wave_in[...]


def solution(mesh):
    cuts, circ = mesh.shape["cuts"], mesh.shape["circ"]

    def shards(sources, inverse, memory, target, weight, decay, initial):
        steps, scen, nodes = sources.shape[1], sources.shape[3], sources.shape[4]
        blocks, ports = weight.shape[1], weight.shape[2]
        rows = steps * scen
        cols = nodes // LANE
        chains, swaps = ITERS + 1, ITERS * SWEEPS
        others = max(circ - 1, 1)
        fused = circ <= 2
        span = steps * ports
        vmem = pl.BlockSpec(memory_space=pltpu.VMEM)
        hbm = pl.BlockSpec(memory_space=pl.ANY)
        dma = pltpu.SemaphoreType.DMA
        square = pltpu.VMEM((nodes, nodes), BF16)
        start, wave = pl.pallas_call(
            functools.partial(kernel, cuts, circ, steps, fused),
            out_shape=(
                jax.ShapeDtypeStruct((scen, nodes), F32),
                jax.ShapeDtypeStruct((rows, nodes), BF16),
            ),
            in_specs=[hbm] * 7,
            out_specs=(vmem, hbm),
            scratch_shapes=[
                pltpu.VMEM((rows, nodes), BF16),
                square,
                pltpu.VMEM((1, nodes), F32),
                pltpu.SMEM((1, blocks), jnp.int32),
                pltpu.VMEM((blocks, ports, nodes), BF16),
                pltpu.VMEM((1, nodes), F32),
                pltpu.VMEM((scen, nodes), F32),
                pltpu.VMEM((rows, nodes), BF16),
                dma((6,)),
                dma((cols,)),
                dma(()),
                square,
                square,
                square,
                square,
                pltpu.VMEM((nodes, circ * ports), BF16),
                pltpu.VMEM((steps * ports, nodes), BF16),
                pltpu.VMEM((circ if fused else 1, span if fused else 8, circ * ports), F32),
                pltpu.VMEM((circ * ports, steps * circ * ports) if fused else (16, LANE), BF16),
                pltpu.VMEM((circ * span, ports) if fused else (span, circ * ports), BF16),
                pltpu.VMEM((rows, nodes), F32),
                pltpu.VMEM((rows, nodes), F32),
                pltpu.VMEM((chains, cols, scen, LANE), F32),
                pltpu.VMEM((chains, cuts, scen, LANE), F32),
                pltpu.VMEM((chains, cuts, scen, LANE), F32),
                pltpu.VMEM((chains, cols, scen, LANE), F32),
                pltpu.VMEM((cuts, 1, LANE), F32),
                pltpu.VMEM((ITERS, circ, scen, circ * ports), F32),
                pltpu.VMEM((ITERS, circ, rows, circ * ports), F32),
                pltpu.VMEM((1, 1, 8, LANE) if fused else (swaps, circ, rows, ports), F32),
                pltpu.VMEM((1, 1, 8, LANE) if fused else (swaps, circ, rows, ports), F32),
                dma((chains, cols)),
                dma((chains, cuts)),
                dma((chains, cuts)),
                dma((chains, cols)),
                dma((cols,)),
                dma((cuts,)),
                dma((others,)),
                dma((circ,)),
                dma((ITERS, others)),
                dma((ITERS, circ)),
                dma((ITERS, others)),
                dma((ITERS, circ)),
                dma((swaps, others)),
                dma((swaps, circ)),
            ],
            compiler_params=pltpu.CompilerParams(
                collective_id=0, has_side_effects=True, vmem_limit_bytes=60 * 1024 * 1024
            ),
            name="parareal",
        )(
            sources.reshape(rows, nodes),
            inverse[0],
            memory.reshape(1, nodes),
            target,
            weight[0],
            decay.reshape(1, nodes),
            initial[0],
        )
        start, wave = pl.pallas_call(
            hand_over,
            out_shape=(
                jax.ShapeDtypeStruct(start.shape, F32),
                jax.ShapeDtypeStruct(wave.shape, BF16),
            ),
            in_specs=[vmem, vmem],
            out_specs=(vmem, vmem),
            name="hand_over",
        )(start, wave)
        return start[None, None], wave.reshape(1, steps, 1, scen, nodes)

    return jax.shard_map(
        shards,
        mesh=mesh,
        in_specs=(
            P("cuts", None, "circ", None, None),
            P("circ", None, None),
            P("cuts", "circ", None),
            P("circ", None),
            P("circ", None, None, None),
            P("cuts", "circ", None),
            P("circ", None, None),
        ),
        out_specs=(P("cuts", "circ", None, None), P("cuts", None, "circ", None, None)),
        check_vma=False,
    )
```

```python
import functools
import math

import jax
import jax.numpy as jnp
from jax import lax
from jax.experimental import pallas as pl
from jax.experimental.pallas import tpu as pltpu
from jax.sharding import PartitionSpec as P

SWEEPS = 3
ITERS = 2
MESH = pl.DeviceIdType.MESH
F32 = jnp.float32
BF16 = jnp.bfloat16
LANE = 128


def dot(a, b):
    return jnp.dot(a.astype(BF16), b.astype(BF16), preferred_element_type=F32)


def kernel(
    cuts,
    circ,
    steps,
    fused,
    src_in,
    inv_in,
    mem_in,
    tgt_in,
    cw_in,
    dec_in,
    init_in,
    start_ref,
    wave_ref,
    src_ref,
    inv_ref,
    mem_ref,
    tgt_ref,
    cw_ref,
    dec_ref,
    init_ref,
    sem_in,
    sem_inv,
    inv_t,
    pow1,
    pow2,
    pow4,
    seen_t,
    resp,
    k_all,
    k_sum,
    k_me,
    own,
    own_seen,
    free,
    terms_buf,
    gather_buf,
    chain_buf,
    state_buf,
    decay_buf,
    origin_buf,
    u_buf,
    y_buf,
    part_buf,
    inflow_buf,
    send1,
    recv1,
    send2,
    recv2,
    send_d,
    recv_d,
    send_o,
    recv_o,
    send_k,
    recv_k,
    send_u,
    recv_u,
    send_y,
    recv_y,
    send_x,
    recv_x,
):
    scope = jax.named_scope
    n = lax.axis_index("cuts")
    me = lax.axis_index("circ")
    nodes = inv_ref.shape[0]
    scen = init_ref.shape[0]
    rows = src_ref.shape[0]
    blocks, ports = cw_ref.shape[0], cw_ref.shape[1]
    cols = nodes // LANE
    base = (cuts - cols) // 2
    piece = n - base
    owner = jnp.logical_and(n >= base, n < base + cols)
    lane = pl.multiple_of(piece * LANE, LANE)
    mine = pl.ds(pl.multiple_of(me * ports, ports), ports)
    swapped = circ % 2 == 0
    mate = me + 1 - 2 * lax.rem(me, 2) if swapped else me
    plane = math.gcd(cuts, 4)
    high = terms_buf.shape[2]
    parts = scen // high
    last = rows - scen
    width = circ * ports
    port_t = seen_t.at[:, 0:width]

    def cut(k):
        return lax.rem(n + k, cuts)

    def peer(k):
        return lax.rem(me + k, circ)

    barrier = pltpu.get_barrier_semaphore()

    @pl.when(owner)
    def _():
        @pl.loop(1, cuts)
        def _(k):
            pl.semaphore_signal(barrier, inc=1, device_id=(cut(k), mate), device_id_type=MESH)

    @pl.when(jnp.logical_not(owner))
    def _():
        for k in range(cols):
            pl.semaphore_signal(barrier, inc=1, device_id=(base + k, mate), device_id_type=MESH)

    for k in range(1, circ):
        pl.semaphore_signal(barrier, inc=1, device_id=(n, peer(k)), device_id_type=MESH)

    def load(k, a, b):
        return pltpu.make_async_copy(a, b, sem_in.at[k])

    first_loads = [load(0, src_in, src_ref), load(1, mem_in, mem_ref)]
    last_loads = [
        load(2, dec_in, dec_ref),
        load(3, tgt_in, tgt_ref),
        load(4, cw_in, cw_ref),
        load(5, init_in, init_ref),
    ]
    strips = []
    for c in range(cols):
        at = pl.ds(c * LANE, LANE)
        strips.append(pltpu.make_async_copy(inv_in.at[at], inv_ref.at[at], sem_inv.at[c]))
    for copy in first_loads + strips + last_loads:
        copy.start()

    def term_copy(e, k, dest):
        return pltpu.make_async_remote_copy(
            src_ref=terms_buf.at[e, k],
            dst_ref=gather_buf.at[e, n],
            send_sem=send1.at[e, k],
            recv_sem=recv1.at[e, n // plane],
            device_id=(dest, mate),
            device_id_type=MESH,
        )

    def decay_copy(k, dest):
        return pltpu.make_async_remote_copy(
            src_ref=dec_ref.at[:, pl.ds(k * LANE, LANE)],
            dst_ref=decay_buf.at[n],
            send_sem=send_d.at[k],
            recv_sem=recv_d,
            device_id=(dest, mate),
            device_id_type=MESH,
        )

    def origin_copy():
        return pltpu.make_async_remote_copy(
            src_ref=init_ref.at[:, pl.ds(lane, LANE)],
            dst_ref=origin_buf,
            send_sem=send_o,
            recv_sem=recv_o,
            device_id=(n, mate),
            device_id_type=MESH,
        )

    def state_copy(e, dest, k):
        return pltpu.make_async_remote_copy(
            src_ref=chain_buf.at[e, dest],
            dst_ref=state_buf.at[e, k],
            send_sem=send2.at[e, dest],
            recv_sem=recv2.at[e, k],
            device_id=(dest, mate),
            device_id_type=MESH,
        )

    def landed(buffer, recv, count):
        return pltpu.make_async_remote_copy(
            src_ref=buffer.at[pl.ds(0, count)],
            dst_ref=buffer.at[pl.ds(0, count)],
            send_sem=send_o,
            recv_sem=recv,
            device_id=(n, mate),
            device_id_type=MESH,
        )

    def apart(other):
        return True if swapped else n != other

    def sends_to(dest):
        return n < cuts - 1 if swapped else jnp.logical_and(n != dest, n < cuts - 1)

    def chain_send(c, terms):
        for h in range(parts):
            for k in range(cols):
                terms_buf[c * parts + h, k] = terms[
                    h * high : (h + 1) * high, k * LANE : (k + 1) * LANE
                ]

        def push(order):
            for e in range(c * parts, (c + 1) * parts):
                for k in order:

                    @pl.when(sends_to(base + k))
                    def _():
                        term_copy(e, k, base + k).start()

        @pl.when(n < cuts // 2)
        def _():
            push(range(cols - 1, -1, -1))

        @pl.when(n >= cuts // 2)
        def _():
            push(range(cols))

    def wait_landed(buffer, recv, first, stop):
        count = min(stop, cuts - 1) - first
        if swapped:
            landed(buffer, recv, count).wait_recv()
        else:
            here = jnp.logical_and(n >= first, n < first + count)

            @pl.when(here)
            def _():
                if count > 1:
                    landed(buffer, recv, count - 1).wait_recv()

            @pl.when(jnp.logical_not(here))
            def _():
                landed(buffer, recv, count).wait_recv()

    def chain_turn(c):
        @pl.when(owner)
        def _():
            if c == 0:
                wait_landed(decay_buf, recv_d, 0, cuts)
                if swapped:
                    origin_copy().wait_recv()
                else:
                    decay_buf[n] = dec_ref[:, pl.ds(lane, LANE)]
                    origin_buf[...] = init_ref[:, pl.ds(lane, LANE)]
            for h in range(parts):
                e = c * parts + h
                if not swapped:
                    gather_buf[e, n] = terms_buf[e, piece]
                state = origin_buf[h * high : (h + 1) * high]
                for s in range(cuts):
                    chain_buf[e, s] = state
                    if s > 0:

                        @pl.when(apart(s))
                        def _():
                            state_copy(e, s, piece).start()

                    if s < cuts - 1:
                        if s % plane == 0:
                            group = recv1.at[e, s // plane]
                            wait_landed(gather_buf.at[e], group, s, s + plane)
                        state = decay_buf[s] * state + gather_buf[e, s]
                if not swapped:
                    state_buf[e, piece] = chain_buf[e, n]

    def chain_end(c):
        blocks = range(c * parts, (c + 1) * parts)
        for e in blocks:
            for k in range(cols):

                @pl.when(jnp.logical_and(apart(base + k), n > 0))
                def _():
                    state_copy(e, 0, k).wait_recv()

        return jnp.concatenate(
            [jnp.concatenate([state_buf[e, k] for k in range(cols)], axis=1) for e in blocks],
            axis=0,
        )

    def drain(c):
        for e in range(c * parts, (c + 1) * parts):
            for k in range(cols):

                @pl.when(sends_to(base + k))
                def _():
                    term_copy(e, k, base + k).wait_send()

        if c == 0:
            for k in range(cols):

                @pl.when(sends_to(base + k))
                def _():
                    decay_copy(k, base + k).wait_send()

        @pl.when(owner)
        def _():
            if c == 0 and swapped:
                origin_copy().wait_send()
            for e in range(c * parts, (c + 1) * parts):
                for s in range(1, cuts):

                    @pl.when(apart(s))
                    def _():
                        state_copy(e, s, piece).wait_send()

    def swap_copy(ref, send, recv, k, source):
        return pltpu.make_async_remote_copy(
            src_ref=ref.at[me],
            dst_ref=ref.at[source],
            send_sem=send.at[k - 1],
            recv_sem=recv.at[source],
            device_id=(n, peer(k)),
            device_id_type=MESH,
        )

    class Swap:
        def __init__(self, *refs):
            self.refs = refs

        def start(self):
            for k in range(1, circ):
                swap_copy(*self.refs, k, me).start()

        def wait(self):
            for k in range(1, circ):
                swap_copy(*self.refs, k, peer(k)).wait_recv()

        def drain(self):
            for k in range(1, circ):
                swap_copy(*self.refs, k, me).wait_send()

    def current_copy(e, height, k, source):
        return pltpu.make_async_remote_copy(
            src_ref=part_buf.at[e, peer(k), pl.ds(0, height)],
            dst_ref=inflow_buf.at[e, source, pl.ds(0, height)],
            send_sem=send_x.at[e, k - 1],
            recv_sem=recv_x.at[e, source],
            device_id=(n, peer(k)),
            device_id_type=MESH,
        )

    def exchange_start(e, partial):
        height = partial.shape[0]
        for g in range(circ):
            part_buf[e, g, 0:height] = partial[:, g * ports : (g + 1) * ports]
        for k in range(1, circ):
            current_copy(e, height, k, me).start()

    def exchange_end(e, height):
        total = part_buf[e, me, 0:height]
        for k in range(1, circ):
            current_copy(e, height, k, peer(k)).wait_recv()
            total = total + inflow_buf[e, peer(k), 0:height]
        return total

    def exchange_drain(e, height):
        for k in range(1, circ):
            current_copy(e, height, k, me).wait_send()

    wide = min(256, nodes)

    def product(out, left, right):
        for at in range(0, nodes, wide):
            out[:, at : at + wide] = dot(left[...], right[:, at : at + wide]).astype(BF16)

    with scope("w_src"):
        for copy in first_loads:
            copy.wait()
    with scope("mean"):
        mean = src_ref[0:scen].astype(F32)
        for t in range(1, steps):
            mean = mean + src_ref[t * scen : (t + 1) * scen].astype(F32)
        mean = mean * (1.0 / steps)
        factor = jnp.broadcast_to(mem_ref[...], (LANE, nodes)).T
    for c in range(cols):
        at = slice(c * LANE, (c + 1) * LANE)
        with scope("w_inv"):
            strips[c].wait()
        turned = inv_ref[at, :].T
        inv_t[:, at] = turned
        pow1[:, at] = (turned.astype(F32) * factor).astype(BF16)
    with scope("w_rest"):
        for copy in last_loads:
            copy.wait()

    @pl.when(n == 0)
    def _():
        for e in range((ITERS + 1) * parts):
            top = e % parts * high
            for k in range(cols):
                state_buf[e, k] = init_ref[top : top + high, k * LANE : (k + 1) * LANE]

    with scope("w_barrier"):

        @pl.when(owner)
        def _():
            pl.semaphore_wait(barrier, cuts - 1 + circ - 1)

        @pl.when(jnp.logical_not(owner))
        def _():
            pl.semaphore_wait(barrier, cols + circ - 1)

    chain_send(0, mean)
    for k in range(cols):

        @pl.when(sends_to(base + k))
        def _():
            decay_copy(k, base + k).start()

    if swapped:

        @pl.when(owner)
        def _():
            origin_copy().start()

    with scope("port_t"):
        for g in range(circ):
            summed = jnp.zeros((ports, nodes), F32)
            for b in range(blocks):
                share = jnp.where(tgt_ref[0, b] == g, 1.0, 0.0).astype(F32)
                summed = summed + share * cw_ref[b].astype(F32)
            port_t[:, g * ports : (g + 1) * ports] = summed.astype(BF16).T

    def one_step(values):
        exact = mem_ref[...] * values
        high = exact.astype(BF16)
        low = (exact - high.astype(F32)).astype(BF16)
        both = dot(jnp.concatenate([high, low], axis=0), inv_t[...])
        return both[: values.shape[0]] + both[values.shape[0] :]

    with scope("pow2"):
        product(pow2, pow1, pow1)
    with scope("own0"):
        own[...] = dot(src_ref[...], inv_t[...])
        resp[0:ports] = inv_t[0:ports]

    with scope("own1"):
        own[scen:] = own[scen:] + one_step(own[: rows - scen])
        resp[ports : 2 * ports] = dot(resp[0:ports], pow1[...]).astype(BF16)

    with scope("turn0"):
        chain_turn(0)

    def beside(left, low, power):
        count = left.shape[0]
        both = dot(jnp.concatenate([left, resp[low * ports : (low + 2) * ports]], axis=0), power)
        resp[(low + 2) * ports : (low + 4) * ports] = both[count:].astype(BF16)
        return both[:count]

    with scope("own2"):
        own[2 * scen :] = own[2 * scen :] + beside(own[: rows - 2 * scen].astype(BF16), 0, pow2[...])
    with scope("own4"):
        ahead = beside(own[: rows - 4 * scen].astype(BF16), 2, pow2[...])
        own[4 * scen :] = own[4 * scen :] + beside(ahead.astype(BF16), 4, pow2[...])

    if fused:
        k_swap = Swap(k_all, send_k, recv_k)
        u_swaps = [Swap(u_buf.at[i], send_u.at[i], recv_u.at[i]) for i in range(ITERS)]
        y_swaps = [Swap(y_buf.at[i], send_y.at[i], recv_y.at[i]) for i in range(ITERS)]

        def take(j):
            total = jnp.zeros((ports, width), F32)
            for t in range(steps):
                total = total + k_all[j, t * ports : (t + 1) * ports]
                k_sum[pl.ds(pl.multiple_of(j * ports, ports), ports), t * width : (t + 1) * width] = (
                    total.astype(BF16)
                )
            span = steps * ports
            k_me[pl.ds(pl.multiple_of(j * span, span), span), :] = k_all[j, :, mine].astype(BF16)

    with scope("port_resp"):
        heard = dot(resp[...], port_t[...])
        if fused:
            k_all[me] = heard
            k_swap.start()
        else:
            k_me[...] = heard.astype(BF16)

    def shifted(low):
        columns = [low]
        for lag in range(1, steps):
            columns.append(
                jnp.concatenate(
                    [jnp.zeros((lag * scen, ports), BF16), low[: rows - lag * scen]], axis=0
                )
            )
        return columns

    def by_lag(currents):
        return jnp.concatenate(shifted(currents.astype(BF16)), axis=1)

    def end_lags(currents):
        low = currents.astype(BF16)
        return jnp.concatenate(
            [low[(steps - 1 - lag) * scen : (steps - lag) * scen] for lag in range(steps)], axis=1
        )

    def keep():
        free[0:scen] = own[0:scen] + v1
        free[scen : 2 * scen] = own[scen : 2 * scen] + v2
        free[2 * scen : 4 * scen] = own[2 * scen : 4 * scen] + v34
        free[4 * scen :] = own[4 * scen :] + v58

    with scope("end0"):
        begin = chain_end(0)
    for iteration in range(ITERS):
        first = iteration * SWEEPS
        with scope("free"):
            v0 = begin.astype(BF16)
            outflow = dot(v0, port_t[...])
            v1 = one_step(begin)
            v2 = dot(v0, pow2[...])
            v12 = jnp.concatenate([v1, v2], axis=0).astype(BF16)
            if fused:
                u_buf[iteration, me] = outflow
                u_swaps[iteration].start()
            else:
                exchange_start(first, outflow)
            if iteration == 0:
                v34 = dot(v12, pow2[...])
                v56 = dot(v34, pow2[...])
                v78 = dot(v56, pow2[...])
                v58 = jnp.concatenate([v56, v78], axis=0)
                keep()
                seen = dot(free[...], port_t[...])
            else:
                heard = dot(v12, seen_t[...])
                pairs = [heard[:, k * width : (k + 1) * width] for k in range(steps // 2)]
                seen = own_seen[...] + jnp.concatenate(pairs, axis=0)
        if fused:
            with scope("y_start"):
                y_buf[iteration, me] = seen
                y_swaps[iteration].start()
            with scope("w_k"):
                if iteration == 0:
                    take(me)
                    k_swap.wait()
                    for k in range(1, circ):
                        take(peer(k))
            if iteration > 0:
                with scope("later"):
                    v34 = dot(v12, pow2[...])
                    v58 = dot(jnp.concatenate([v12, v34.astype(BF16)], axis=0), pow4[...])
                    free[last:] = own[last:] + v58[3 * scen :]
            with scope("w_u"):
                u_swaps[iteration].wait()
            with scope("ku"):
                inflow = outflow
                for k in range(1, circ):
                    inflow = inflow + u_buf[iteration, peer(k)]
                raised = dot(inflow, k_sum[...])
                raised = jnp.concatenate(
                    [raised[:, t * width : (t + 1) * width] for t in range(steps)], axis=0
                )
            with scope("w_y"):
                y_swaps[iteration].wait()
            with scope("sweep"):
                total = seen
                direct = y_buf[iteration, me, :, mine]
                for k in range(1, circ):
                    total = total + y_buf[iteration, peer(k)]
                    direct = direct + y_buf[iteration, peer(k), :, mine]
                second = (total + raised).astype(BF16)
                columns = []
                for g in range(circ):
                    columns += shifted(second[:, g * ports : (g + 1) * ports])
                current = direct + dot(jnp.concatenate(columns, axis=1), k_me[...])
        else:
            if iteration > 0:
                v34 = dot(v12, pow2[...])
                v58 = dot(jnp.concatenate([v12, v34.astype(BF16)], axis=0), pow4[...])
                free[last:] = own[last:] + v58[3 * scen :]
            current = exchange_end(first, scen)
            current = jnp.concatenate([current] * steps, axis=0)
            for sweep in range(1, SWEEPS):
                exchange_start(first + sweep, seen + dot(by_lag(current), k_me[...]))
                current = exchange_end(first + sweep, rows)
        with scope("final"):
            final = free[last:] + dot(end_lags(current), resp[...])
        with scope("send"):
            chain_send(iteration + 1, final - dec_ref[...] * begin)
        if iteration < ITERS - 1:
            with scope("pow4"):
                product(pow4, pow2, pow2)
                seen_t[:, width : 2 * width] = dot(pow2[...], port_t[...]).astype(BF16)
                own_seen[...] = dot(own[...], port_t[...])
        else:
            with scope("wave"):
                keep()
                wave = free[...] + dot(by_lag(current), resp[...])
                wave_ref[...] = wave.astype(BF16)
        with scope("turn"):
            chain_turn(iteration + 1)
        if iteration < ITERS - 1:
            with scope("seen_t"):
                half = seen_t[:, 0 : 2 * width]
                seen_t[:, 2 * width : 4 * width] = dot(pow4[...], half).astype(BF16)
        with scope("end"):
            begin = chain_end(iteration + 1)
    with scope("out"):
        start_ref[...] = begin

    with scope("drain"):
        for c in range(ITERS + 1):
            drain(c)
        if fused:
            k_swap.drain()
            for swap in u_swaps + y_swaps:
                swap.drain()
        else:
            for e in range(SWEEPS * ITERS):
                exchange_drain(e, scen if e % SWEEPS == 0 else rows)


def hand_over(start_in, wave_in, start_out, wave_out, sems):
    copies = [
        pltpu.make_async_copy(start_in, start_out, sems.at[0]),
        pltpu.make_async_copy(wave_in, wave_out, sems.at[1]),
    ]
    for copy in copies:
        copy.start()
    for copy in copies:
        copy.wait()


def solution(mesh):
    cuts, circ = mesh.shape["cuts"], mesh.shape["circ"]

    def shards(sources, inverse, memory, target, weight, decay, initial):
        steps, scen, nodes = sources.shape[1], sources.shape[3], sources.shape[4]
        blocks, ports = weight.shape[1], weight.shape[2]
        rows = steps * scen
        cols = nodes // LANE
        high = scen
        chains, swaps = (ITERS + 1) * (scen // high), ITERS * SWEEPS
        others = max(circ - 1, 1)
        fused = circ <= 2
        span = steps * ports
        vmem = pl.BlockSpec(memory_space=pltpu.VMEM)
        hbm = pl.BlockSpec(memory_space=pl.ANY)
        dma = pltpu.SemaphoreType.DMA
        square = pltpu.VMEM((nodes, nodes), BF16)
        start, wave = pl.pallas_call(
            functools.partial(kernel, cuts, circ, steps, fused),
            out_shape=(pltpu.VMEM((scen, nodes), F32), pltpu.VMEM((rows, nodes), BF16)),
            in_specs=[hbm] * 7,
            out_specs=(vmem, vmem),
            scratch_shapes=[
                pltpu.VMEM((rows, nodes), BF16),
                square,
                pltpu.VMEM((1, nodes), F32),
                pltpu.SMEM((1, blocks), jnp.int32),
                pltpu.VMEM((blocks, ports, nodes), BF16),
                pltpu.VMEM((1, nodes), F32),
                pltpu.VMEM((scen, nodes), F32),
                dma((6,)),
                dma((cols,)),
                square,
                square,
                square,
                square,
                pltpu.VMEM((nodes, steps // 2 * circ * ports), BF16),
                pltpu.VMEM((steps * ports, nodes), BF16),
                pltpu.VMEM((circ if fused else 1, span if fused else 8, circ * ports), F32),
                pltpu.VMEM((circ * ports, steps * circ * ports) if fused else (16, LANE), BF16),
                pltpu.VMEM((circ * span, ports) if fused else (span, circ * ports), BF16),
                pltpu.VMEM((rows, nodes), F32),
                pltpu.VMEM((rows, circ * ports), F32),
                pltpu.VMEM((rows, nodes), F32),
                pltpu.VMEM((chains, cols, high, LANE), F32),
                pltpu.VMEM((chains, cuts, high, LANE), F32),
                pltpu.VMEM((chains, cuts, high, LANE), F32),
                pltpu.VMEM((chains, cols, high, LANE), F32),
                pltpu.VMEM((cuts, 1, LANE), F32),
                pltpu.VMEM((scen, LANE), F32),
                pltpu.VMEM((ITERS, circ, scen, circ * ports), F32),
                pltpu.VMEM((ITERS, circ, rows, circ * ports), F32),
                pltpu.VMEM((1, 1, 8, LANE) if fused else (swaps, circ, rows, ports), F32),
                pltpu.VMEM((1, 1, 8, LANE) if fused else (swaps, circ, rows, ports), F32),
                dma((chains, cols)),
                dma((chains, cuts)),
                dma((chains, cuts)),
                dma((chains, cols)),
                dma((cols,)),
                dma(()),
                dma(()),
                dma(()),
                dma((others,)),
                dma((circ,)),
                dma((ITERS, others)),
                dma((ITERS, circ)),
                dma((ITERS, others)),
                dma((ITERS, circ)),
                dma((swaps, others)),
                dma((swaps, circ)),
            ],
            compiler_params=pltpu.CompilerParams(
                collective_id=0, has_side_effects=True, vmem_limit_bytes=60 * 1024 * 1024
            ),
            name="parareal",
        )(
            sources.reshape(rows, nodes),
            inverse[0],
            memory.reshape(1, nodes),
            target,
            weight[0],
            decay.reshape(1, nodes),
            initial[0],
        )
        start, wave = (pltpu.with_memory_space_constraint(x, pltpu.VMEM) for x in (start, wave))
        start, wave = pl.pallas_call(
            hand_over,
            out_shape=(
                jax.ShapeDtypeStruct(start.shape, F32),
                jax.ShapeDtypeStruct(wave.shape, BF16),
            ),
            in_specs=[vmem, vmem],
            out_specs=(hbm, hbm),
            scratch_shapes=[dma((2,))],
            name="hand_over",
        )(start, wave)
        return start[None, None], wave.reshape(1, steps, 1, scen, nodes)

    return jax.shard_map(
        shards,
        mesh=mesh,
        in_specs=(
            P("cuts", None, "circ", None, None),
            P("circ", None, None),
            P("cuts", "circ", None),
            P("circ", None),
            P("circ", None, None, None),
            P("cuts", "circ", None),
            P("circ", None, None),
        ),
        out_specs=(P("cuts", "circ", None, None), P("cuts", None, "circ", None, None)),
        check_vma=False,
    )
```

```python
import functools
import math

import jax
import jax.numpy as jnp
from jax import lax
from jax.experimental import pallas as pl
from jax.experimental.pallas import tpu as pltpu
from jax.sharding import PartitionSpec as P

SWEEPS = 3
ITERS = 2
MESH = pl.DeviceIdType.MESH
F32 = jnp.float32
BF16 = jnp.bfloat16
LANE = 128


def dot(a, b):
    return jnp.dot(a.astype(BF16), b.astype(BF16), preferred_element_type=F32)


def kernel(
    cuts,
    circ,
    steps,
    fused,
    src_in,
    inv_in,
    mem_in,
    tgt_in,
    cw_in,
    dec_in,
    init_in,
    start_ref,
    wave_ref,
    src_ref,
    inv_ref,
    mem_ref,
    tgt_ref,
    cw_ref,
    dec_ref,
    init_ref,
    sem_in,
    sem_inv,
    inv_t,
    pow1,
    pow2,
    pow4,
    seen_t,
    resp,
    k_all,
    k_sum,
    k_me,
    own,
    own_seen,
    free,
    terms_buf,
    gather_buf,
    chain_buf,
    state_buf,
    decay_buf,
    origin_buf,
    near_buf,
    near_chain,
    near_dec,
    near_prod,
    side_buf,
    scale_buf,
    u_buf,
    y_buf,
    part_buf,
    inflow_buf,
    send1,
    recv1,
    send2,
    recv2,
    send_d,
    recv_d,
    send_o,
    recv_o,
    send_n1,
    recv_n1,
    send_n2,
    recv_n2,
    send_nd,
    recv_nd,
    send_np,
    recv_np,
    send_k,
    recv_k,
    send_u,
    recv_u,
    send_y,
    recv_y,
    send_x,
    recv_x,
):
    scope = jax.named_scope
    n = lax.axis_index("cuts")
    me = lax.axis_index("circ")
    nodes = inv_ref.shape[0]
    scen = init_ref.shape[0]
    rows = src_ref.shape[0]
    blocks, ports = cw_ref.shape[0], cw_ref.shape[1]
    cols = nodes // LANE
    base = (cuts - cols) // 2
    piece = n - base
    owner = jnp.logical_and(n >= base, n < base + cols)
    lane = pl.multiple_of(piece * LANE, LANE)
    mine = pl.ds(pl.multiple_of(me * ports, ports), ports)
    swapped = circ % 2 == 0
    mate = me + 1 - 2 * lax.rem(me, 2) if swapped else me
    plane = math.gcd(cuts, 4)
    high = terms_buf.shape[2]
    parts = scen // high
    last = rows - scen
    width = circ * ports
    port_t = seen_t.at[:, 0:width]

    near = swapped and 1 < plane <= base and cols % plane == 0
    per = cols // plane
    tail = cuts - plane if near else cuts - 1
    edge = jnp.logical_or(n < plane, n >= cuts - plane)
    rim = jnp.where(n < plane, 0, cuts - plane)
    rank = n - rim
    behind = jnp.logical_and(edge, rank > 0)
    ahead_of = jnp.logical_and(edge, rank < plane - 1)

    def cut(k):
        return lax.rem(n + k, cuts)

    def peer(k):
        return lax.rem(me + k, circ)

    barrier = pltpu.get_barrier_semaphore()

    @pl.when(owner)
    def _():
        @pl.loop(1, cuts)
        def _(k):
            pl.semaphore_signal(barrier, inc=1, device_id=(cut(k), mate), device_id_type=MESH)

    @pl.when(jnp.logical_not(owner))
    def _():
        for k in range(cols):
            pl.semaphore_signal(barrier, inc=1, device_id=(base + k, mate), device_id_type=MESH)

    if near:

        @pl.when(edge)
        def _():
            for k in range(1, plane):
                other = rim + lax.rem(rank + k, plane)
                pl.semaphore_signal(barrier, inc=1, device_id=(other, mate), device_id_type=MESH)

    for k in range(1, circ):
        pl.semaphore_signal(barrier, inc=1, device_id=(n, peer(k)), device_id_type=MESH)

    def load(k, a, b):
        return pltpu.make_async_copy(a, b, sem_in.at[k])

    first_loads = [load(0, src_in, src_ref), load(1, mem_in, mem_ref)]
    last_loads = [
        load(2, dec_in, dec_ref),
        load(3, tgt_in, tgt_ref),
        load(4, cw_in, cw_ref),
        load(5, init_in, init_ref),
    ]
    strips = []
    for c in range(cols):
        at = pl.ds(c * LANE, LANE)
        strips.append(pltpu.make_async_copy(inv_in.at[at], inv_ref.at[at], sem_inv.at[c]))
    for copy in first_loads + strips + last_loads:
        copy.start()

    def term_copy(e, k, dest):
        return pltpu.make_async_remote_copy(
            src_ref=terms_buf.at[e, k],
            dst_ref=gather_buf.at[e, n],
            send_sem=send1.at[e, k],
            recv_sem=recv1.at[e, n // plane],
            device_id=(dest, mate),
            device_id_type=MESH,
        )

    def decay_copy(k, dest):
        return pltpu.make_async_remote_copy(
            src_ref=dec_ref.at[:, pl.ds(k * LANE, LANE)],
            dst_ref=decay_buf.at[n],
            send_sem=send_d.at[k],
            recv_sem=recv_d,
            device_id=(dest, mate),
            device_id_type=MESH,
        )

    def origin_copy():
        return pltpu.make_async_remote_copy(
            src_ref=init_ref.at[:, pl.ds(lane, LANE)],
            dst_ref=origin_buf,
            send_sem=send_o,
            recv_sem=recv_o,
            device_id=(n, mate),
            device_id_type=MESH,
        )

    def near_term(c, q):
        return pltpu.make_async_remote_copy(
            src_ref=terms_buf.at[c, pl.ds(q * per, per)],
            dst_ref=near_buf.at[c, rank],
            send_sem=send_n1.at[c, q],
            recv_sem=recv_n1.at[c],
            device_id=(rim + q, mate),
            device_id_type=MESH,
        )

    def near_decay(q):
        return pltpu.make_async_remote_copy(
            src_ref=dec_ref.at[:, pl.ds(q * per * LANE, per * LANE)],
            dst_ref=near_dec.at[rank],
            send_sem=send_nd.at[q],
            recv_sem=recv_nd,
            device_id=(rim + q, mate),
            device_id_type=MESH,
        )

    def near_scale(t, q):
        return pltpu.make_async_remote_copy(
            src_ref=near_prod.at[t],
            dst_ref=scale_buf.at[:, pl.ds(q * per * LANE, per * LANE)],
            send_sem=send_np.at[t],
            recv_sem=recv_np.at[q],
            device_id=(rim + t, mate),
            device_id_type=MESH,
        )

    def near_state(c, t, q):
        return pltpu.make_async_remote_copy(
            src_ref=near_chain.at[c, t],
            dst_ref=side_buf.at[c, pl.ds(q * per, per)],
            send_sem=send_n2.at[c, t],
            recv_sem=recv_n2.at[c, q],
            device_id=(rim + t, mate),
            device_id_type=MESH,
        )

    def near_send(c):
        if near:

            @pl.when(ahead_of)
            def _():
                for q in range(plane):
                    near_term(c, q).start()
                    if c == 0:
                        near_decay(q).start()

    def near_turn(c):
        if near:

            @pl.when(edge)
            def _():
                if c == 0:
                    landed(near_dec, recv_nd, plane - 1).wait_recv()
                    rate = near_dec[0]
                    for t in range(1, plane):
                        near_prod[t] = rate
                        if t < plane - 1:
                            rate = rate * near_dec[t]
                landed(near_buf.at[c], recv_n1.at[c], plane - 1).wait_recv()
                states = [near_buf[c, 0, p] for p in range(per)]
                for t in range(1, plane):
                    for p in range(per):
                        near_chain[c, t, p] = states[p]
                        if t < plane - 1:
                            rate = near_dec[t, :, p * LANE : (p + 1) * LANE]
                            states[p] = rate * states[p] + near_buf[c, t, p]
                for t in range(1, plane):
                    for q in range(plane):

                        @pl.when(rank == q)
                        def _():
                            near_state(c, t, q).start()
                            if c == 0:
                                near_scale(t, q).start()

    def near_drain(c):
        if near:

            @pl.when(ahead_of)
            def _():
                for q in range(plane):
                    near_term(c, q).wait_send()
                    if c == 0:
                        near_decay(q).wait_send()

            @pl.when(edge)
            def _():
                for t in range(1, plane):
                    near_state(c, t, 0).wait_send()
                    if c == 0:
                        near_scale(t, 0).wait_send()

    nearest = plane if near else 1

    def state_copy(e, dest, k):
        return pltpu.make_async_remote_copy(
            src_ref=chain_buf.at[e, dest],
            dst_ref=state_buf.at[e, k],
            send_sem=send2.at[e, dest],
            recv_sem=recv2.at[e, k],
            device_id=(dest, mate),
            device_id_type=MESH,
        )

    def landed(buffer, recv, count):
        return pltpu.make_async_remote_copy(
            src_ref=buffer.at[pl.ds(0, count)],
            dst_ref=buffer.at[pl.ds(0, count)],
            send_sem=send_o,
            recv_sem=recv,
            device_id=(n, mate),
            device_id_type=MESH,
        )

    def apart(other):
        return True if swapped else n != other

    def sends_to(dest):
        return n < tail if swapped else jnp.logical_and(n != dest, n < cuts - 1)

    def chain_send(c, terms):
        for h in range(parts):
            for k in range(cols):
                terms_buf[c * parts + h, k] = terms[
                    h * high : (h + 1) * high, k * LANE : (k + 1) * LANE
                ]

        def push(order):
            for e in range(c * parts, (c + 1) * parts):
                for k in order:

                    @pl.when(sends_to(base + k))
                    def _():
                        term_copy(e, k, base + k).start()

        @pl.when(n < cuts // 2)
        def _():
            push(range(cols - 1, -1, -1))

        @pl.when(n >= cuts // 2)
        def _():
            push(range(cols))

        near_send(c)

    def wait_landed(buffer, recv, first, stop):
        count = min(stop, tail) - first
        if swapped:
            landed(buffer, recv, count).wait_recv()
        else:
            here = jnp.logical_and(n >= first, n < first + count)

            @pl.when(here)
            def _():
                if count > 1:
                    landed(buffer, recv, count - 1).wait_recv()

            @pl.when(jnp.logical_not(here))
            def _():
                landed(buffer, recv, count).wait_recv()

    def chain_turn(c):
        @pl.when(owner)
        def _():
            if c == 0:
                wait_landed(decay_buf, recv_d, 0, cuts)
                if swapped:
                    origin_copy().wait_recv()
                else:
                    decay_buf[n] = dec_ref[:, pl.ds(lane, LANE)]
                    origin_buf[...] = init_ref[:, pl.ds(lane, LANE)]
            for h in range(parts):
                e = c * parts + h
                if not swapped:
                    gather_buf[e, n] = terms_buf[e, piece]
                state = origin_buf[h * high : (h + 1) * high]
                for s in range(cuts):
                    chain_buf[e, s] = state
                    if s >= nearest:

                        @pl.when(apart(s))
                        def _():
                            state_copy(e, s, piece).start()

                    if s < tail:
                        if s % plane == 0:
                            group = recv1.at[e, s // plane]
                            wait_landed(gather_buf.at[e], group, s, s + plane)
                        state = decay_buf[s] * state + gather_buf[e, s]
                if not swapped:
                    state_buf[e, piece] = chain_buf[e, n]

    def chain_end(c):
        blocks = range(c * parts, (c + 1) * parts)
        for e in blocks:
            for k in range(cols):

                @pl.when(jnp.logical_and(apart(base + k), n >= nearest))
                def _():
                    state_copy(e, 0, k).wait_recv()

        begin = jnp.concatenate(
            [jnp.concatenate([state_buf[e, k] for k in range(cols)], axis=1) for e in blocks],
            axis=0,
        )
        if near:

            @pl.when(behind)
            def _():
                for q in range(plane):
                    near_state(c, 1, q).wait_recv()
                    if c == 0:
                        near_scale(1, q).wait_recv()

            side = jnp.concatenate([side_buf[c, k] for k in range(cols)], axis=1)
            begin = scale_buf[...] * begin + side
        return begin

    def drain(c):
        for e in range(c * parts, (c + 1) * parts):
            for k in range(cols):

                @pl.when(sends_to(base + k))
                def _():
                    term_copy(e, k, base + k).wait_send()

        if c == 0:
            for k in range(cols):

                @pl.when(sends_to(base + k))
                def _():
                    decay_copy(k, base + k).wait_send()

        @pl.when(owner)
        def _():
            if c == 0 and swapped:
                origin_copy().wait_send()
            for e in range(c * parts, (c + 1) * parts):
                for s in range(nearest, cuts):

                    @pl.when(apart(s))
                    def _():
                        state_copy(e, s, piece).wait_send()

    def swap_copy(ref, send, recv, k, source):
        return pltpu.make_async_remote_copy(
            src_ref=ref.at[me],
            dst_ref=ref.at[source],
            send_sem=send.at[k - 1],
            recv_sem=recv.at[source],
            device_id=(n, peer(k)),
            device_id_type=MESH,
        )

    class Swap:
        def __init__(self, *refs):
            self.refs = refs

        def start(self):
            for k in range(1, circ):
                swap_copy(*self.refs, k, me).start()

        def wait(self):
            for k in range(1, circ):
                swap_copy(*self.refs, k, peer(k)).wait_recv()

        def drain(self):
            for k in range(1, circ):
                swap_copy(*self.refs, k, me).wait_send()

    def current_copy(e, height, k, source):
        return pltpu.make_async_remote_copy(
            src_ref=part_buf.at[e, peer(k), pl.ds(0, height)],
            dst_ref=inflow_buf.at[e, source, pl.ds(0, height)],
            send_sem=send_x.at[e, k - 1],
            recv_sem=recv_x.at[e, source],
            device_id=(n, peer(k)),
            device_id_type=MESH,
        )

    def exchange_start(e, partial):
        height = partial.shape[0]
        for g in range(circ):
            part_buf[e, g, 0:height] = partial[:, g * ports : (g + 1) * ports]
        for k in range(1, circ):
            current_copy(e, height, k, me).start()

    def exchange_end(e, height):
        total = part_buf[e, me, 0:height]
        for k in range(1, circ):
            current_copy(e, height, k, peer(k)).wait_recv()
            total = total + inflow_buf[e, peer(k), 0:height]
        return total

    def exchange_drain(e, height):
        for k in range(1, circ):
            current_copy(e, height, k, me).wait_send()

    wide = min(256, nodes)

    def product(out, left, right):
        for at in range(0, nodes, wide):
            out[:, at : at + wide] = dot(left[...], right[:, at : at + wide]).astype(BF16)

    with scope("w_src"):
        for copy in first_loads:
            copy.wait()
    with scope("mean"):
        mean = src_ref[0:scen].astype(F32)
        for t in range(1, steps):
            mean = mean + src_ref[t * scen : (t + 1) * scen].astype(F32)
        mean = mean * (1.0 / steps)
        factor = jnp.broadcast_to(mem_ref[...], (LANE, nodes)).T
    for c in range(cols):
        at = slice(c * LANE, (c + 1) * LANE)
        with scope("w_inv"):
            strips[c].wait()
        turned = inv_ref[at, :].T
        inv_t[:, at] = turned
        pow1[:, at] = (turned.astype(F32) * factor).astype(BF16)
    with scope("w_rest"):
        for copy in last_loads:
            copy.wait()

    if near:

        @pl.when(jnp.logical_not(behind))
        def _():
            side_buf[...] = jnp.zeros_like(side_buf)
            scale_buf[...] = jnp.ones_like(scale_buf)

    @pl.when(n < nearest)
    def _():
        for e in range((ITERS + 1) * parts):
            top = e % parts * high
            for k in range(cols):
                state_buf[e, k] = init_ref[top : top + high, k * LANE : (k + 1) * LANE]

    with scope("w_barrier"):

        @pl.when(owner)
        def _():
            pl.semaphore_wait(barrier, cuts - 1 + circ - 1)

        if near:

            @pl.when(edge)
            def _():
                pl.semaphore_wait(barrier, cols + circ - 1 + plane - 1)

        @pl.when(jnp.logical_not(jnp.logical_or(owner, edge) if near else owner))
        def _():
            pl.semaphore_wait(barrier, cols + circ - 1)

    chain_send(0, mean)
    for k in range(cols):

        @pl.when(sends_to(base + k))
        def _():
            decay_copy(k, base + k).start()

    if swapped:

        @pl.when(owner)
        def _():
            origin_copy().start()


    with scope("port_t"):
        for g in range(circ):
            summed = jnp.zeros((ports, nodes), F32)
            for b in range(blocks):
                share = jnp.where(tgt_ref[0, b] == g, 1.0, 0.0).astype(F32)
                summed = summed + share * cw_ref[b].astype(F32)
            port_t[:, g * ports : (g + 1) * ports] = summed.astype(BF16).T

    def one_step(values):
        exact = mem_ref[...] * values
        high = exact.astype(BF16)
        low = (exact - high.astype(F32)).astype(BF16)
        both = dot(jnp.concatenate([high, low], axis=0), inv_t[...])
        return both[: values.shape[0]] + both[values.shape[0] :]

    with scope("pow2"):
        product(pow2, pow1, pow1)
    with scope("own0"):
        own[...] = dot(src_ref[...], inv_t[...])
        resp[0:ports] = inv_t[0:ports]

    with scope("own1"):
        own[scen:] = own[scen:] + one_step(own[: rows - scen])
        resp[ports : 2 * ports] = dot(resp[0:ports], pow1[...]).astype(BF16)

    with scope("turn0"):
        near_turn(0)
        chain_turn(0)

    def beside(left, low, power):
        count = left.shape[0]
        both = dot(jnp.concatenate([left, resp[low * ports : (low + 2) * ports]], axis=0), power)
        resp[(low + 2) * ports : (low + 4) * ports] = both[count:].astype(BF16)
        return both[:count]

    with scope("own2"):
        own[2 * scen :] = own[2 * scen :] + beside(own[: rows - 2 * scen].astype(BF16), 0, pow2[...])
    with scope("own4"):
        ahead = beside(own[: rows - 4 * scen].astype(BF16), 2, pow2[...])
        own[4 * scen :] = own[4 * scen :] + beside(ahead.astype(BF16), 4, pow2[...])

    if fused:
        k_swap = Swap(k_all, send_k, recv_k)
        u_swaps = [Swap(u_buf.at[i], send_u.at[i], recv_u.at[i]) for i in range(ITERS)]
        y_swaps = [Swap(y_buf.at[i], send_y.at[i], recv_y.at[i]) for i in range(ITERS)]

        def take(j):
            total = jnp.zeros((ports, width), F32)
            for t in range(steps):
                total = total + k_all[j, t * ports : (t + 1) * ports]
                k_sum[pl.ds(pl.multiple_of(j * ports, ports), ports), t * width : (t + 1) * width] = (
                    total.astype(BF16)
                )
            span = steps * ports
            k_me[pl.ds(pl.multiple_of(j * span, span), span), :] = k_all[j, :, mine].astype(BF16)

    with scope("port_resp"):
        heard = dot(resp[...], port_t[...])
        if fused:
            k_all[me] = heard
            k_swap.start()
        else:
            k_me[...] = heard.astype(BF16)

    def shifted(low):
        columns = [low]
        for lag in range(1, steps):
            columns.append(
                jnp.concatenate(
                    [jnp.zeros((lag * scen, ports), BF16), low[: rows - lag * scen]], axis=0
                )
            )
        return columns

    def by_lag(currents):
        return jnp.concatenate(shifted(currents.astype(BF16)), axis=1)

    def end_lags(currents):
        low = currents.astype(BF16)
        return jnp.concatenate(
            [low[(steps - 1 - lag) * scen : (steps - lag) * scen] for lag in range(steps)], axis=1
        )

    def keep():
        free[0:scen] = own[0:scen] + v1
        free[scen : 2 * scen] = own[scen : 2 * scen] + v2
        free[2 * scen : 4 * scen] = own[2 * scen : 4 * scen] + v34
        free[4 * scen :] = own[4 * scen :] + v58

    with scope("end0"):
        begin = chain_end(0)
    for iteration in range(ITERS):
        first = iteration * SWEEPS
        with scope("free"):
            start_ref[...] = begin
            v0 = begin.astype(BF16)
            if iteration == 0:
                outflow = dot(v0, port_t[...])
                v1 = one_step(begin)
                v2 = dot(v0, pow2[...])
            else:
                v4 = dot(v0, pow4[...]).astype(BF16)
                heard = dot(jnp.concatenate([v0, v4], axis=0), seen_t[...])
                outflow = heard[0:scen, 0:width]
            if fused:
                u_buf[iteration, me] = outflow
                u_swaps[iteration].start()
            else:
                exchange_start(first, outflow)
            if iteration == 0:
                v12 = jnp.concatenate([v1, v2], axis=0).astype(BF16)
                v34 = dot(v12, pow2[...])
                v56 = dot(v34, pow2[...])
                v78 = dot(v56, pow2[...])
                v58 = jnp.concatenate([v56, v78], axis=0)
                keep()
                ending = free[last:]
                seen = dot(free[...], port_t[...])
            else:
                slabs = [
                    heard[r * scen : (r + 1) * scen, k * width : (k + 1) * width]
                    for r in range(2)
                    for k in range(1, steps // 2 + 1)
                ]
                seen = own_seen[...] + jnp.concatenate(slabs, axis=0)
        if fused:
            with scope("y_start"):
                y_buf[iteration, me] = seen
                y_swaps[iteration].start()
            with scope("w_k"):
                if iteration == 0:
                    take(me)
                    k_swap.wait()
                    for k in range(1, circ):
                        take(peer(k))
            if iteration > 0:
                with scope("later"):
                    ending = own[last:] + dot(v4, pow4[...])
            with scope("w_u"):
                u_swaps[iteration].wait()
            with scope("ku"):
                inflow = outflow
                for k in range(1, circ):
                    inflow = inflow + u_buf[iteration, peer(k)]
                raised = dot(inflow, k_sum[...])
                raised = jnp.concatenate(
                    [raised[:, t * width : (t + 1) * width] for t in range(steps)], axis=0
                )
            with scope("w_y"):
                y_swaps[iteration].wait()
            with scope("sweep"):
                total = seen
                direct = y_buf[iteration, me, :, mine]
                for k in range(1, circ):
                    total = total + y_buf[iteration, peer(k)]
                    direct = direct + y_buf[iteration, peer(k), :, mine]
                second = (total + raised).astype(BF16)
                columns = []
                for g in range(circ):
                    columns += shifted(second[:, g * ports : (g + 1) * ports])
                current = direct + dot(jnp.concatenate(columns, axis=1), k_me[...])
        else:
            if iteration > 0:
                ending = own[last:] + dot(v4, pow4[...])
            current = exchange_end(first, scen)
            current = jnp.concatenate([current] * steps, axis=0)
            for sweep in range(1, SWEEPS):
                exchange_start(first + sweep, seen + dot(by_lag(current), k_me[...]))
                current = exchange_end(first + sweep, rows)
        with scope("final"):
            final = ending + dot(end_lags(current), resp[...])
        with scope("send"):
            chain_send(iteration + 1, final - dec_ref[...] * start_ref[...])
        if iteration < ITERS - 1:
            with scope("pow4"):
                product(pow4, pow2, pow2)
            with scope("near"):
                near_turn(iteration + 1)
            with scope("seen"):
                seen_t[:, width : 2 * width] = dot(pow1[...], port_t[...]).astype(BF16)
                own_seen[...] = dot(own[...], port_t[...])
        else:
            with scope("wave"):
                v1 = one_step(start_ref[...])
                v2 = dot(start_ref[...], pow2[...])
                v12 = jnp.concatenate([v1, v2], axis=0).astype(BF16)
                v34 = dot(v12, pow2[...])
                v58 = dot(jnp.concatenate([v12, v34.astype(BF16)], axis=0), pow4[...])
                keep()
                wave = free[...] + dot(by_lag(current), resp[...])
                wave_ref[...] = wave.astype(BF16)
            with scope("near"):
                near_turn(iteration + 1)
        with scope("turn"):
            chain_turn(iteration + 1)
        if iteration < ITERS - 1:
            with scope("seen_t"):
                seen_t[:, 2 * width : 3 * width] = dot(pow2[...], port_t[...]).astype(BF16)
                half = seen_t[:, width : 3 * width]
                seen_t[:, 3 * width : 5 * width] = dot(pow2[...], half).astype(BF16)
        with scope("end"):
            begin = chain_end(iteration + 1)
    with scope("out"):
        start_ref[...] = begin

    with scope("drain"):
        for c in range(ITERS + 1):
            drain(c)
            near_drain(c)
        if fused:
            k_swap.drain()
            for swap in u_swaps + y_swaps:
                swap.drain()
        else:
            for e in range(SWEEPS * ITERS):
                exchange_drain(e, scen if e % SWEEPS == 0 else rows)


def hand_over(start_in, wave_in, start_out, wave_out, sems):
    copies = [
        pltpu.make_async_copy(start_in, start_out, sems.at[0]),
        pltpu.make_async_copy(wave_in, wave_out, sems.at[1]),
    ]
    for copy in copies:
        copy.start()
    for copy in copies:
        copy.wait()


def solution(mesh):
    cuts, circ = mesh.shape["cuts"], mesh.shape["circ"]

    def shards(sources, inverse, memory, target, weight, decay, initial):
        steps, scen, nodes = sources.shape[1], sources.shape[3], sources.shape[4]
        blocks, ports = weight.shape[1], weight.shape[2]
        rows = steps * scen
        cols = nodes // LANE
        high = scen
        plane = math.gcd(cuts, 4)
        per = max(cols // plane, 1)
        chains, swaps = (ITERS + 1) * (scen // high), ITERS * SWEEPS
        others = max(circ - 1, 1)
        fused = circ <= 2
        span = steps * ports
        vmem = pl.BlockSpec(memory_space=pltpu.VMEM)
        hbm = pl.BlockSpec(memory_space=pl.ANY)
        dma = pltpu.SemaphoreType.DMA
        square = pltpu.VMEM((nodes, nodes), BF16)
        start, wave = pl.pallas_call(
            functools.partial(kernel, cuts, circ, steps, fused),
            out_shape=(pltpu.VMEM((scen, nodes), F32), pltpu.VMEM((rows, nodes), BF16)),
            in_specs=[hbm] * 7,
            out_specs=(vmem, vmem),
            scratch_shapes=[
                pltpu.VMEM((rows, nodes), BF16),
                square,
                pltpu.VMEM((1, nodes), F32),
                pltpu.SMEM((1, blocks), jnp.int32),
                pltpu.VMEM((blocks, ports, nodes), BF16),
                pltpu.VMEM((1, nodes), F32),
                pltpu.VMEM((scen, nodes), F32),
                dma((6,)),
                dma((cols,)),
                square,
                square,
                square,
                square,
                pltpu.VMEM((nodes, (steps // 2 + 1) * circ * ports), BF16),
                pltpu.VMEM((steps * ports, nodes), BF16),
                pltpu.VMEM((circ if fused else 1, span if fused else 8, circ * ports), F32),
                pltpu.VMEM((circ * ports, steps * circ * ports) if fused else (16, LANE), BF16),
                pltpu.VMEM((circ * span, ports) if fused else (span, circ * ports), BF16),
                pltpu.VMEM((rows, nodes), F32),
                pltpu.VMEM((rows, circ * ports), F32),
                pltpu.VMEM((rows, nodes), F32),
                pltpu.VMEM((chains, cols, high, LANE), F32),
                pltpu.VMEM((chains, cuts, high, LANE), F32),
                pltpu.VMEM((chains, cuts, high, LANE), F32),
                pltpu.VMEM((chains, cols, high, LANE), F32),
                pltpu.VMEM((cuts, 1, LANE), F32),
                pltpu.VMEM((scen, LANE), F32),
                pltpu.VMEM((chains, plane, per, scen, LANE), F32),
                pltpu.VMEM((chains, plane, per, scen, LANE), F32),
                pltpu.VMEM((plane, 1, per * LANE), F32),
                pltpu.VMEM((plane, 1, per * LANE), F32),
                pltpu.VMEM((chains, cols, scen, LANE), F32),
                pltpu.VMEM((1, nodes), F32),
                pltpu.VMEM((ITERS, circ, scen, circ * ports), F32),
                pltpu.VMEM((ITERS, circ, rows, circ * ports), F32),
                pltpu.VMEM((1, 1, 8, LANE) if fused else (swaps, circ, rows, ports), F32),
                pltpu.VMEM((1, 1, 8, LANE) if fused else (swaps, circ, rows, ports), F32),
                dma((chains, cols)),
                dma((chains, cuts)),
                dma((chains, cuts)),
                dma((chains, cols)),
                dma((cols,)),
                dma(()),
                dma(()),
                dma(()),
                dma((chains, plane)),
                dma((chains,)),
                dma((chains, plane)),
                dma((chains, plane)),
                dma((plane,)),
                dma(()),
                dma((plane,)),
                dma((plane,)),
                dma((others,)),
                dma((circ,)),
                dma((ITERS, others)),
                dma((ITERS, circ)),
                dma((ITERS, others)),
                dma((ITERS, circ)),
                dma((swaps, others)),
                dma((swaps, circ)),
            ],
            compiler_params=pltpu.CompilerParams(
                collective_id=0, has_side_effects=True, vmem_limit_bytes=60 * 1024 * 1024
            ),
            name="parareal",
        )(
            sources.reshape(rows, nodes),
            inverse[0],
            memory.reshape(1, nodes),
            target,
            weight[0],
            decay.reshape(1, nodes),
            initial[0],
        )
        start, wave = (pltpu.with_memory_space_constraint(x, pltpu.VMEM) for x in (start, wave))
        start, wave = pl.pallas_call(
            hand_over,
            out_shape=(
                jax.ShapeDtypeStruct(start.shape, F32),
                jax.ShapeDtypeStruct(wave.shape, BF16),
            ),
            in_specs=[vmem, vmem],
            out_specs=(hbm, hbm),
            scratch_shapes=[dma((2,))],
            name="hand_over",
        )(start, wave)
        return start[None, None], wave.reshape(1, steps, 1, scen, nodes)

    return jax.shard_map(
        shards,
        mesh=mesh,
        in_specs=(
            P("cuts", None, "circ", None, None),
            P("circ", None, None),
            P("cuts", "circ", None),
            P("circ", None),
            P("circ", None, None, None),
            P("cuts", "circ", None),
            P("circ", None, None),
        ),
        out_specs=(P("cuts", "circ", None, None), P("cuts", None, "circ", None, None)),
        check_vma=False,
    )
```

```python
import functools
import math

import jax
import jax.numpy as jnp
from jax import lax
from jax.experimental import pallas as pl
from jax.experimental.pallas import tpu as pltpu
from jax.sharding import PartitionSpec as P

SWEEPS = 3
ITERS = 2
MESH = pl.DeviceIdType.MESH
F32 = jnp.float32
BF16 = jnp.bfloat16
LANE = 128


def dot(a, b):
    return jnp.dot(a.astype(BF16), b.astype(BF16), preferred_element_type=F32)


def kernel(
    cuts,
    circ,
    steps,
    fused,
    src_in,
    inv_in,
    mem_in,
    tgt_in,
    cw_in,
    dec_in,
    init_in,
    start_ref,
    wave_ref,
    src_ref,
    inv_ref,
    mem_ref,
    tgt_ref,
    cw_ref,
    dec_ref,
    init_ref,
    sem_in,
    sem_inv,
    inv_t,
    pow1,
    pow2,
    pow4,
    seen_t,
    resp,
    k_all,
    k_sum,
    k_me,
    own,
    own_seen,
    free,
    terms_buf,
    gather_buf,
    chain_buf,
    state_buf,
    decay_buf,
    origin_buf,
    near_buf,
    near_chain,
    near_dec,
    near_prod,
    side_buf,
    scale_buf,
    u_buf,
    y_buf,
    part_buf,
    inflow_buf,
    send1,
    recv1,
    send2,
    recv2,
    send_d,
    recv_d,
    send_o,
    recv_o,
    send_n1,
    recv_n1,
    send_n2,
    recv_n2,
    send_nd,
    recv_nd,
    send_np,
    recv_np,
    send_k,
    recv_k,
    send_u,
    recv_u,
    send_y,
    recv_y,
    send_x,
    recv_x,
):
    scope = jax.named_scope
    n = lax.axis_index("cuts")
    me = lax.axis_index("circ")
    nodes = inv_ref.shape[0]
    scen = init_ref.shape[0]
    rows = src_ref.shape[0]
    blocks, ports = cw_ref.shape[0], cw_ref.shape[1]
    cols = nodes // LANE
    base = (cuts - cols) // 2
    piece = n - base
    owner = jnp.logical_and(n >= base, n < base + cols)
    lane = pl.multiple_of(piece * LANE, LANE)
    mine = pl.ds(pl.multiple_of(me * ports, ports), ports)
    swapped = circ % 2 == 0
    mate = me + 1 - 2 * lax.rem(me, 2) if swapped else me
    plane = math.gcd(cuts, 4)
    high = terms_buf.shape[2]
    parts = scen // high
    last = rows - scen
    width = circ * ports
    port_t = seen_t.at[:, 0:width]

    near = swapped and 1 < plane <= base and cols % plane == 0
    per = cols // plane
    tail = cuts - plane if near else cuts - 1
    edge = jnp.logical_or(n < plane, n >= cuts - plane)
    rim = jnp.where(n < plane, 0, cuts - plane)
    rank = n - rim
    behind = jnp.logical_and(edge, rank > 0)
    ahead_of = jnp.logical_and(edge, rank < plane - 1)

    def cut(k):
        return lax.rem(n + k, cuts)

    def peer(k):
        return lax.rem(me + k, circ)

    barrier = pltpu.get_barrier_semaphore()

    @pl.when(owner)
    def _():
        @pl.loop(1, cuts)
        def _(k):
            pl.semaphore_signal(barrier, inc=1, device_id=(cut(k), mate), device_id_type=MESH)

    @pl.when(jnp.logical_not(owner))
    def _():
        for k in range(cols):
            pl.semaphore_signal(barrier, inc=1, device_id=(base + k, mate), device_id_type=MESH)

    if near:

        @pl.when(edge)
        def _():
            for k in range(1, plane):
                other = rim + lax.rem(rank + k, plane)
                pl.semaphore_signal(barrier, inc=1, device_id=(other, mate), device_id_type=MESH)

    for k in range(1, circ):
        pl.semaphore_signal(barrier, inc=1, device_id=(n, peer(k)), device_id_type=MESH)

    def load(k, a, b):
        return pltpu.make_async_copy(a, b, sem_in.at[k])

    first_loads = [load(0, src_in, src_ref), load(1, mem_in, mem_ref)]
    last_loads = [
        load(2, dec_in, dec_ref),
        load(3, tgt_in, tgt_ref),
        load(4, cw_in, cw_ref),
        load(5, init_in, init_ref),
    ]
    strips = []
    batch = math.gcd(cols, 4)
    for c in range(cols // batch):
        at = pl.ds(c * batch * LANE, batch * LANE)
        strips.append(pltpu.make_async_copy(inv_in.at[at], inv_ref.at[at], sem_inv.at[c]))
    for copy in first_loads + strips + last_loads:
        copy.start()

    def term_copy(e, k, dest):
        return pltpu.make_async_remote_copy(
            src_ref=terms_buf.at[e, k],
            dst_ref=gather_buf.at[e, n],
            send_sem=send1.at[e, k],
            recv_sem=recv1.at[e, n // plane],
            device_id=(dest, mate),
            device_id_type=MESH,
        )

    def decay_copy(k, dest):
        return pltpu.make_async_remote_copy(
            src_ref=dec_ref.at[:, pl.ds(k * LANE, LANE)],
            dst_ref=decay_buf.at[n],
            send_sem=send_d.at[k],
            recv_sem=recv_d,
            device_id=(dest, mate),
            device_id_type=MESH,
        )

    def origin_copy():
        return pltpu.make_async_remote_copy(
            src_ref=init_ref.at[:, pl.ds(lane, LANE)],
            dst_ref=origin_buf,
            send_sem=send_o,
            recv_sem=recv_o,
            device_id=(n, mate),
            device_id_type=MESH,
        )

    def near_term(c, q):
        return pltpu.make_async_remote_copy(
            src_ref=terms_buf.at[c, pl.ds(q * per, per)],
            dst_ref=near_buf.at[c, rank],
            send_sem=send_n1.at[c, q],
            recv_sem=recv_n1.at[c],
            device_id=(rim + q, mate),
            device_id_type=MESH,
        )

    def near_decay(q):
        return pltpu.make_async_remote_copy(
            src_ref=dec_ref.at[:, pl.ds(q * per * LANE, per * LANE)],
            dst_ref=near_dec.at[rank],
            send_sem=send_nd.at[q],
            recv_sem=recv_nd,
            device_id=(rim + q, mate),
            device_id_type=MESH,
        )

    def near_scale(t, q):
        return pltpu.make_async_remote_copy(
            src_ref=near_prod.at[t],
            dst_ref=scale_buf.at[:, pl.ds(q * per * LANE, per * LANE)],
            send_sem=send_np.at[t],
            recv_sem=recv_np.at[q],
            device_id=(rim + t, mate),
            device_id_type=MESH,
        )

    def near_state(c, t, q):
        return pltpu.make_async_remote_copy(
            src_ref=near_chain.at[c, t],
            dst_ref=side_buf.at[c, pl.ds(q * per, per)],
            send_sem=send_n2.at[c, t],
            recv_sem=recv_n2.at[c, q],
            device_id=(rim + t, mate),
            device_id_type=MESH,
        )

    def near_send(c):
        if near:

            @pl.when(ahead_of)
            def _():
                for q in range(plane):
                    near_term(c, q).start()
                    if c == 0:
                        near_decay(q).start()

    def near_turn(c):
        if near:

            @pl.when(edge)
            def _():
                if c == 0:
                    landed(near_dec, recv_nd, plane - 1).wait_recv()
                    rate = near_dec[0]
                    for t in range(1, plane):
                        near_prod[t] = rate
                        if t < plane - 1:
                            rate = rate * near_dec[t]
                landed(near_buf.at[c], recv_n1.at[c], plane - 1).wait_recv()
                states = [near_buf[c, 0, p] for p in range(per)]
                for t in range(1, plane):
                    for p in range(per):
                        near_chain[c, t, p] = states[p]
                        if t < plane - 1:
                            rate = near_dec[t, :, p * LANE : (p + 1) * LANE]
                            states[p] = rate * states[p] + near_buf[c, t, p]
                for t in range(1, plane):
                    for q in range(plane):

                        @pl.when(rank == q)
                        def _():
                            near_state(c, t, q).start()
                            if c == 0:
                                near_scale(t, q).start()

    def near_drain(c):
        if near:

            @pl.when(ahead_of)
            def _():
                for q in range(plane):
                    near_term(c, q).wait_send()
                    if c == 0:
                        near_decay(q).wait_send()

            @pl.when(edge)
            def _():
                for t in range(1, plane):
                    near_state(c, t, 0).wait_send()
                    if c == 0:
                        near_scale(t, 0).wait_send()

    nearest = plane if near else 1

    def state_copy(e, dest, k):
        return pltpu.make_async_remote_copy(
            src_ref=chain_buf.at[e, dest],
            dst_ref=state_buf.at[e, k],
            send_sem=send2.at[e, dest],
            recv_sem=recv2.at[e, k],
            device_id=(dest, mate),
            device_id_type=MESH,
        )

    def landed(buffer, recv, count):
        return pltpu.make_async_remote_copy(
            src_ref=buffer.at[pl.ds(0, count)],
            dst_ref=buffer.at[pl.ds(0, count)],
            send_sem=send_o,
            recv_sem=recv,
            device_id=(n, mate),
            device_id_type=MESH,
        )

    def apart(other):
        return True if swapped else n != other

    def sends_to(dest):
        return n < tail if swapped else jnp.logical_and(n != dest, n < cuts - 1)

    def chain_send(c, terms):
        for h in range(parts):
            for k in range(cols):
                terms_buf[c * parts + h, k] = terms[
                    h * high : (h + 1) * high, k * LANE : (k + 1) * LANE
                ]

        def push(order):
            for e in range(c * parts, (c + 1) * parts):
                for k in order:

                    @pl.when(sends_to(base + k))
                    def _():
                        term_copy(e, k, base + k).start()

        @pl.when(n < cuts // 2)
        def _():
            push(range(cols - 1, -1, -1))

        @pl.when(n >= cuts // 2)
        def _():
            push(range(cols))

        near_send(c)

    def wait_landed(buffer, recv, first, stop):
        count = min(stop, tail) - first
        if swapped:
            landed(buffer, recv, count).wait_recv()
        else:
            here = jnp.logical_and(n >= first, n < first + count)

            @pl.when(here)
            def _():
                if count > 1:
                    landed(buffer, recv, count - 1).wait_recv()

            @pl.when(jnp.logical_not(here))
            def _():
                landed(buffer, recv, count).wait_recv()

    def chain_turn(c):
        @pl.when(owner)
        def _():
            if c == 0:
                wait_landed(decay_buf, recv_d, 0, cuts)
                if swapped:
                    origin_copy().wait_recv()
                else:
                    decay_buf[n] = dec_ref[:, pl.ds(lane, LANE)]
                    origin_buf[...] = init_ref[:, pl.ds(lane, LANE)]
            for h in range(parts):
                e = c * parts + h
                if not swapped:
                    gather_buf[e, n] = terms_buf[e, piece]
                state = origin_buf[h * high : (h + 1) * high]
                for s in range(cuts):
                    chain_buf[e, s] = state
                    if s >= nearest:

                        @pl.when(apart(s))
                        def _():
                            state_copy(e, s, piece).start()

                    if s < tail:
                        if s % plane == 0:
                            group = recv1.at[e, s // plane]
                            wait_landed(gather_buf.at[e], group, s, s + plane)
                        state = decay_buf[s] * state + gather_buf[e, s]
                if not swapped:
                    state_buf[e, piece] = chain_buf[e, n]

    def chain_end(c):
        blocks = range(c * parts, (c + 1) * parts)
        for e in blocks:
            for k in range(cols):

                @pl.when(jnp.logical_and(apart(base + k), n >= nearest))
                def _():
                    state_copy(e, 0, k).wait_recv()

        begin = jnp.concatenate(
            [jnp.concatenate([state_buf[e, k] for k in range(cols)], axis=1) for e in blocks],
            axis=0,
        )
        if near:

            @pl.when(behind)
            def _():
                for q in range(plane):
                    near_state(c, 1, q).wait_recv()
                    if c == 0:
                        near_scale(1, q).wait_recv()

            side = jnp.concatenate([side_buf[c, k] for k in range(cols)], axis=1)
            begin = scale_buf[...] * begin + side
        return begin

    def drain(c):
        for e in range(c * parts, (c + 1) * parts):
            for k in range(cols):

                @pl.when(sends_to(base + k))
                def _():
                    term_copy(e, k, base + k).wait_send()

        if c == 0:
            for k in range(cols):

                @pl.when(sends_to(base + k))
                def _():
                    decay_copy(k, base + k).wait_send()

        @pl.when(owner)
        def _():
            if c == 0 and swapped:
                origin_copy().wait_send()
            for e in range(c * parts, (c + 1) * parts):
                for s in range(nearest, cuts):

                    @pl.when(apart(s))
                    def _():
                        state_copy(e, s, piece).wait_send()

    def swap_copy(ref, send, recv, k, source):
        return pltpu.make_async_remote_copy(
            src_ref=ref.at[me],
            dst_ref=ref.at[source],
            send_sem=send.at[k - 1],
            recv_sem=recv.at[source],
            device_id=(n, peer(k)),
            device_id_type=MESH,
        )

    class Swap:
        def __init__(self, *refs):
            self.refs = refs

        def start(self):
            for k in range(1, circ):
                swap_copy(*self.refs, k, me).start()

        def wait(self):
            for k in range(1, circ):
                swap_copy(*self.refs, k, peer(k)).wait_recv()

        def drain(self):
            for k in range(1, circ):
                swap_copy(*self.refs, k, me).wait_send()

    def current_copy(e, height, k, source):
        return pltpu.make_async_remote_copy(
            src_ref=part_buf.at[e, peer(k), pl.ds(0, height)],
            dst_ref=inflow_buf.at[e, source, pl.ds(0, height)],
            send_sem=send_x.at[e, k - 1],
            recv_sem=recv_x.at[e, source],
            device_id=(n, peer(k)),
            device_id_type=MESH,
        )

    def exchange_start(e, partial):
        height = partial.shape[0]
        for g in range(circ):
            part_buf[e, g, 0:height] = partial[:, g * ports : (g + 1) * ports]
        for k in range(1, circ):
            current_copy(e, height, k, me).start()

    def exchange_end(e, height):
        total = part_buf[e, me, 0:height]
        for k in range(1, circ):
            current_copy(e, height, k, peer(k)).wait_recv()
            total = total + inflow_buf[e, peer(k), 0:height]
        return total

    def exchange_drain(e, height):
        for k in range(1, circ):
            current_copy(e, height, k, me).wait_send()

    wide = min(256, nodes)

    def product(out, left, right):
        for at in range(0, nodes, wide):
            out[:, at : at + wide] = dot(left[...], right[:, at : at + wide]).astype(BF16)

    with scope("w_src"):
        for copy in first_loads:
            copy.wait()
    with scope("mean"):
        mean = src_ref[0:scen].astype(F32)
        for t in range(1, steps):
            mean = mean + src_ref[t * scen : (t + 1) * scen].astype(F32)
        mean = mean * (1.0 / steps)
        factor = jnp.broadcast_to(mem_ref[...], (LANE, nodes)).T
    for c in range(cols):
        at = slice(c * LANE, (c + 1) * LANE)
        if c % batch == 0:
            with scope("w_inv"):
                strips[c // batch].wait()
        turned = inv_ref[at, :].T
        inv_t[:, at] = turned
        pow1[:, at] = (turned.astype(F32) * factor).astype(BF16)
    with scope("w_rest"):
        for copy in last_loads:
            copy.wait()

    if near:

        @pl.when(jnp.logical_not(behind))
        def _():
            side_buf[...] = jnp.zeros_like(side_buf)
            scale_buf[...] = jnp.ones_like(scale_buf)

    @pl.when(n < nearest)
    def _():
        for e in range((ITERS + 1) * parts):
            top = e % parts * high
            for k in range(cols):
                state_buf[e, k] = init_ref[top : top + high, k * LANE : (k + 1) * LANE]

    with scope("w_barrier"):

        @pl.when(owner)
        def _():
            pl.semaphore_wait(barrier, cuts - 1 + circ - 1)

        if near:

            @pl.when(edge)
            def _():
                pl.semaphore_wait(barrier, cols + circ - 1 + plane - 1)

        @pl.when(jnp.logical_not(jnp.logical_or(owner, edge) if near else owner))
        def _():
            pl.semaphore_wait(barrier, cols + circ - 1)

    chain_send(0, mean)
    for k in range(cols):

        @pl.when(sends_to(base + k))
        def _():
            decay_copy(k, base + k).start()

    if swapped:

        @pl.when(owner)
        def _():
            origin_copy().start()


    with scope("port_t"):
        for g in range(circ):
            summed = jnp.zeros((ports, nodes), F32)
            for b in range(blocks):
                share = jnp.where(tgt_ref[0, b] == g, 1.0, 0.0).astype(F32)
                summed = summed + share * cw_ref[b].astype(F32)
            port_t[:, g * ports : (g + 1) * ports] = summed.astype(BF16).T

    def one_step(values):
        exact = mem_ref[...] * values
        high = exact.astype(BF16)
        low = (exact - high.astype(F32)).astype(BF16)
        both = dot(jnp.concatenate([high, low], axis=0), inv_t[...])
        return both[: values.shape[0]] + both[values.shape[0] :]

    with scope("pow2"):
        product(pow2, pow1, pow1)
    with scope("own0"):
        own[...] = dot(src_ref[...], inv_t[...])
        resp[0:ports] = inv_t[0:ports]

    with scope("own1"):
        own[scen:] = own[scen:] + dot(mem_ref[...] * own[: rows - scen], inv_t[...])
        resp[ports : 2 * ports] = dot(resp[0:ports], pow1[...]).astype(BF16)

    with scope("turn0"):
        near_turn(0)
        chain_turn(0)

    def beside(left, low, power):
        count = left.shape[0]
        both = dot(jnp.concatenate([left, resp[low * ports : (low + 2) * ports]], axis=0), power)
        resp[(low + 2) * ports : (low + 4) * ports] = both[count:].astype(BF16)
        return both[:count]

    with scope("own2"):
        own[2 * scen :] = own[2 * scen :] + beside(own[: rows - 2 * scen].astype(BF16), 0, pow2[...])
    with scope("own4"):
        ahead = beside(own[: rows - 4 * scen].astype(BF16), 2, pow2[...])
        own[4 * scen :] = own[4 * scen :] + beside(ahead.astype(BF16), 4, pow2[...])

    if fused:
        k_swap = Swap(k_all, send_k, recv_k)
        u_swaps = [Swap(u_buf.at[i], send_u.at[i], recv_u.at[i]) for i in range(ITERS)]
        y_swaps = [Swap(y_buf.at[i], send_y.at[i], recv_y.at[i]) for i in range(ITERS)]

        def take(j):
            total = jnp.zeros((ports, width), F32)
            for t in range(steps):
                total = total + k_all[j, t * ports : (t + 1) * ports]
                k_sum[pl.ds(pl.multiple_of(j * ports, ports), ports), t * width : (t + 1) * width] = (
                    total.astype(BF16)
                )
            span = steps * ports
            k_me[pl.ds(pl.multiple_of(j * span, span), span), :] = k_all[j, :, mine].astype(BF16)

    with scope("port_resp"):
        heard = dot(resp[...], port_t[...])
        if fused:
            k_all[me] = heard
            k_swap.start()
        else:
            k_me[...] = heard.astype(BF16)

    def shifted(low):
        columns = [low]
        for lag in range(1, steps):
            columns.append(
                jnp.concatenate(
                    [jnp.zeros((lag * scen, ports), BF16), low[: rows - lag * scen]], axis=0
                )
            )
        return columns

    def by_lag(currents):
        return jnp.concatenate(shifted(currents.astype(BF16)), axis=1)

    def end_lags(currents):
        low = currents.astype(BF16)
        return jnp.concatenate(
            [low[(steps - 1 - lag) * scen : (steps - lag) * scen] for lag in range(steps)], axis=1
        )

    def keep():
        free[0:scen] = own[0:scen] + v1
        free[scen : 2 * scen] = own[scen : 2 * scen] + v2
        free[2 * scen : 4 * scen] = own[2 * scen : 4 * scen] + v34
        free[4 * scen :] = own[4 * scen :] + v58

    with scope("end0"):
        begin = chain_end(0)
    for iteration in range(ITERS):
        first = iteration * SWEEPS
        with scope("free"):
            start_ref[...] = begin
            v0 = begin.astype(BF16)
            if iteration == 0:
                outflow = dot(v0, port_t[...])
                v1 = one_step(begin)
                v2 = dot(v0, pow2[...])
            else:
                v4 = dot(v0, pow4[...]).astype(BF16)
                heard = dot(jnp.concatenate([v0, v4], axis=0), seen_t[...])
                outflow = heard[0:scen, 0:width]
            if fused:
                u_buf[iteration, me] = outflow
                u_swaps[iteration].start()
            else:
                exchange_start(first, outflow)
            if iteration == 0:
                v12 = jnp.concatenate([v1, v2], axis=0).astype(BF16)
                v34 = dot(v12, pow2[...])
                v56 = dot(v34, pow2[...])
                v78 = dot(v56, pow2[...])
                v58 = jnp.concatenate([v56, v78], axis=0)
                keep()
                ending = free[last:]
                seen = dot(free[...], port_t[...])
            else:
                slabs = [
                    heard[r * scen : (r + 1) * scen, k * width : (k + 1) * width]
                    for r in range(2)
                    for k in range(1, steps // 2 + 1)
                ]
                seen = own_seen[...] + jnp.concatenate(slabs, axis=0)
        if fused:
            with scope("y_start"):
                y_buf[iteration, me] = seen
                y_swaps[iteration].start()
            with scope("w_k"):
                if iteration == 0:
                    take(me)
                    k_swap.wait()
                    for k in range(1, circ):
                        take(peer(k))
            if iteration > 0:
                with scope("later"):
                    ending = own[last:] + dot(v4, pow4[...])
            with scope("w_u"):
                u_swaps[iteration].wait()
            with scope("ku"):
                inflow = outflow
                for k in range(1, circ):
                    inflow = inflow + u_buf[iteration, peer(k)]
                raised = dot(inflow, k_sum[...])
                raised = jnp.concatenate(
                    [raised[:, t * width : (t + 1) * width] for t in range(steps)], axis=0
                )
            with scope("w_y"):
                y_swaps[iteration].wait()
            with scope("sweep"):
                total = seen
                direct = y_buf[iteration, me, :, mine]
                for k in range(1, circ):
                    total = total + y_buf[iteration, peer(k)]
                    direct = direct + y_buf[iteration, peer(k), :, mine]
                second = (total + raised).astype(BF16)
                columns = []
                for g in range(circ):
                    columns += shifted(second[:, g * ports : (g + 1) * ports])
                current = direct + dot(jnp.concatenate(columns, axis=1), k_me[...])
        else:
            if iteration > 0:
                ending = own[last:] + dot(v4, pow4[...])
            current = exchange_end(first, scen)
            current = jnp.concatenate([current] * steps, axis=0)
            for sweep in range(1, SWEEPS):
                exchange_start(first + sweep, seen + dot(by_lag(current), k_me[...]))
                current = exchange_end(first + sweep, rows)
        with scope("final"):
            final = ending + dot(end_lags(current), resp[...])
        with scope("send"):
            chain_send(iteration + 1, final - dec_ref[...] * start_ref[...])
        if iteration < ITERS - 1:
            with scope("pow4"):
                product(pow4, pow2, pow2)
            with scope("near"):
                near_turn(iteration + 1)
            with scope("seen"):
                seen_t[:, width : 2 * width] = dot(pow1[...], port_t[...]).astype(BF16)
                own_seen[...] = dot(own[...], port_t[...])
        else:
            with scope("wave"):
                v1 = one_step(start_ref[...])
                v2 = dot(start_ref[...], pow2[...])
                v12 = jnp.concatenate([v1, v2], axis=0).astype(BF16)
                v34 = dot(v12, pow2[...])
                v58 = dot(jnp.concatenate([v12, v34.astype(BF16)], axis=0), pow4[...])
                keep()
                wave = free[...] + dot(by_lag(current), resp[...])
                wave_ref[...] = wave.astype(BF16)
            with scope("near"):
                near_turn(iteration + 1)
        with scope("turn"):
            chain_turn(iteration + 1)
        if iteration < ITERS - 1:
            with scope("seen_t"):
                seen_t[:, 2 * width : 3 * width] = dot(pow2[...], port_t[...]).astype(BF16)
                half = seen_t[:, width : 3 * width]
                seen_t[:, 3 * width : 5 * width] = dot(pow2[...], half).astype(BF16)
        with scope("end"):
            begin = chain_end(iteration + 1)
    with scope("out"):
        start_ref[...] = begin

    with scope("drain"):
        for c in range(ITERS + 1):
            drain(c)
            near_drain(c)
        if fused:
            k_swap.drain()
            for swap in u_swaps + y_swaps:
                swap.drain()
        else:
            for e in range(SWEEPS * ITERS):
                exchange_drain(e, scen if e % SWEEPS == 0 else rows)


def hand_over(start_in, wave_in, start_out, wave_out, sems):
    copies = [
        pltpu.make_async_copy(start_in, start_out, sems.at[0]),
        pltpu.make_async_copy(wave_in, wave_out, sems.at[1]),
    ]
    for copy in copies:
        copy.start()
    for copy in copies:
        copy.wait()


def solution(mesh):
    cuts, circ = mesh.shape["cuts"], mesh.shape["circ"]

    def shards(sources, inverse, memory, target, weight, decay, initial):
        steps, scen, nodes = sources.shape[1], sources.shape[3], sources.shape[4]
        blocks, ports = weight.shape[1], weight.shape[2]
        rows = steps * scen
        cols = nodes // LANE
        high = scen
        plane = math.gcd(cuts, 4)
        per = max(cols // plane, 1)
        chains, swaps = (ITERS + 1) * (scen // high), ITERS * SWEEPS
        others = max(circ - 1, 1)
        fused = circ <= 2
        span = steps * ports
        vmem = pl.BlockSpec(memory_space=pltpu.VMEM)
        hbm = pl.BlockSpec(memory_space=pl.ANY)
        dma = pltpu.SemaphoreType.DMA
        square = pltpu.VMEM((nodes, nodes), BF16)
        start, wave = pl.pallas_call(
            functools.partial(kernel, cuts, circ, steps, fused),
            out_shape=(pltpu.VMEM((scen, nodes), F32), pltpu.VMEM((rows, nodes), BF16)),
            in_specs=[hbm] * 7,
            out_specs=(vmem, vmem),
            scratch_shapes=[
                pltpu.VMEM((rows, nodes), BF16),
                square,
                pltpu.VMEM((1, nodes), F32),
                pltpu.SMEM((1, blocks), jnp.int32),
                pltpu.VMEM((blocks, ports, nodes), BF16),
                pltpu.VMEM((1, nodes), F32),
                pltpu.VMEM((scen, nodes), F32),
                dma((6,)),
                dma((cols,)),
                square,
                square,
                square,
                square,
                pltpu.VMEM((nodes, (steps // 2 + 1) * circ * ports), BF16),
                pltpu.VMEM((steps * ports, nodes), BF16),
                pltpu.VMEM((circ if fused else 1, span if fused else 8, circ * ports), F32),
                pltpu.VMEM((circ * ports, steps * circ * ports) if fused else (16, LANE), BF16),
                pltpu.VMEM((circ * span, ports) if fused else (span, circ * ports), BF16),
                pltpu.VMEM((rows, nodes), F32),
                pltpu.VMEM((rows, circ * ports), F32),
                pltpu.VMEM((rows, nodes), F32),
                pltpu.VMEM((chains, cols, high, LANE), F32),
                pltpu.VMEM((chains, cuts, high, LANE), F32),
                pltpu.VMEM((chains, cuts, high, LANE), F32),
                pltpu.VMEM((chains, cols, high, LANE), F32),
                pltpu.VMEM((cuts, 1, LANE), F32),
                pltpu.VMEM((scen, LANE), F32),
                pltpu.VMEM((chains, plane, per, scen, LANE), F32),
                pltpu.VMEM((chains, plane, per, scen, LANE), F32),
                pltpu.VMEM((plane, 1, per * LANE), F32),
                pltpu.VMEM((plane, 1, per * LANE), F32),
                pltpu.VMEM((chains, cols, scen, LANE), F32),
                pltpu.VMEM((1, nodes), F32),
                pltpu.VMEM((ITERS, circ, scen, circ * ports), F32),
                pltpu.VMEM((ITERS, circ, rows, circ * ports), F32),
                pltpu.VMEM((1, 1, 8, LANE) if fused else (swaps, circ, rows, ports), F32),
                pltpu.VMEM((1, 1, 8, LANE) if fused else (swaps, circ, rows, ports), F32),
                dma((chains, cols)),
                dma((chains, cuts)),
                dma((chains, cuts)),
                dma((chains, cols)),
                dma((cols,)),
                dma(()),
                dma(()),
                dma(()),
                dma((chains, plane)),
                dma((chains,)),
                dma((chains, plane)),
                dma((chains, plane)),
                dma((plane,)),
                dma(()),
                dma((plane,)),
                dma((plane,)),
                dma((others,)),
                dma((circ,)),
                dma((ITERS, others)),
                dma((ITERS, circ)),
                dma((ITERS, others)),
                dma((ITERS, circ)),
                dma((swaps, others)),
                dma((swaps, circ)),
            ],
            compiler_params=pltpu.CompilerParams(
                collective_id=0, has_side_effects=True, vmem_limit_bytes=60 * 1024 * 1024
            ),
            name="parareal",
        )(
            sources.reshape(rows, nodes),
            inverse[0],
            memory.reshape(1, nodes),
            target,
            weight[0],
            decay.reshape(1, nodes),
            initial[0],
        )
        start, wave = (pltpu.with_memory_space_constraint(x, pltpu.VMEM) for x in (start, wave))
        start, wave = pl.pallas_call(
            hand_over,
            out_shape=(
                jax.ShapeDtypeStruct(start.shape, F32),
                jax.ShapeDtypeStruct(wave.shape, BF16),
            ),
            in_specs=[vmem, vmem],
            out_specs=(hbm, hbm),
            scratch_shapes=[dma((2,))],
            name="hand_over",
        )(start, wave)
        return start[None, None], wave.reshape(1, steps, 1, scen, nodes)

    return jax.shard_map(
        shards,
        mesh=mesh,
        in_specs=(
            P("cuts", None, "circ", None, None),
            P("circ", None, None),
            P("cuts", "circ", None),
            P("circ", None),
            P("circ", None, None, None),
            P("cuts", "circ", None),
            P("circ", None, None),
        ),
        out_specs=(P("cuts", "circ", None, None), P("cuts", None, "circ", None, None)),
        check_vma=False,
    )
```
